32 devices in a mesh: parts: 2 (over x), rows: 16 (over z, y, core).
Axes of the slice: x: 2, y: 2, z: 4, core: 2. Of those that a mesh axis runs over, the one named last changes fastest.
Arguments:
- features: bfloat16 [128, 256, 512], P(('parts', 'rows')), parts along dimension 0, may hold values from -10 to 10, as said below
- grad_out: bfloat16 [128, 256, 512], P(('parts', 'rows')), parts along dimension 0, may hold values from -11 to 11, as said below
- filters: bfloat16 [512, 3, 3, 512], replicated, may hold values from -0.09375 to 0.09375
- norm_gain: float32 [512], replicated, may hold values from 0.25 to 1.75
- norm_bias: float32 [512], replicated, may hold values from -1 to 1
Outputs:
- grad_in: bfloat16 [128, 256, 512], P(('parts', 'rows')), parts along dimension 0
- filter_grad: float32 [1024, 3, 3, 512], P(('parts', 'rows')), parts along dimension 0
- gain_grad: float32 [1024], P('parts'), parts along dimension 0
- bias_grad: float32 [1024], P('parts'), parts along dimension 0
The draws below stay inside these ranges and needn't reach their ends.
There are 2 independent parts, one for each index of `parts`. The reference program is written for one: setup_inputs(seed, part) draws one part's arguments, and reference() takes and returns one part's arrays. A program takes and returns all parts, laid end to end along the dimension named above; an argument that names none is the same for every part. Nothing has to cross between parts.
Inputs may be any that keep to these rules, and one draw needn't show every extreme that they name: `features`: each image row has its own offset and spread for each group. `grad_out`: each image row and channel has its own offset.
All inputs are finite; a program needn't handle non-finite values.
Results may differ from the reference program's by a relative error of at most 0.0005.
Values may be sent and summed in bfloat16 or wider, within the bound.
A program may use at most 128 MiB of HBM per device.

```python
import math
import jax
import jax.numpy as jnp
from jax import lax

C = 512
GROUPS = 32
COLS = 256
HEIGHT = 64


def draw_features(key, part):
    key_noise = jax.random.fold_in(key, 11)
    key_offset = jax.random.fold_in(key, 12)
    key_spread = jax.random.fold_in(key, 13)
    normal_draw = jnp.clip(jax.random.normal(key_noise, (HEIGHT, COLS, C), jnp.float32), -4.0, 4.0)
    offset = jax.random.uniform(key_offset, (HEIGHT, 1, GROUPS), jnp.float32, -1.0, 1.0)
    spread = jnp.exp(jax.random.uniform(key_spread, (HEIGHT, 1, GROUPS), jnp.float32, math.log(0.5), math.log(2.0)))
    offset = jnp.repeat(offset, C // GROUPS, axis=2)
    spread = jnp.repeat(spread, C // GROUPS, axis=2)
    return (offset + spread * normal_draw).astype(jnp.bfloat16)


def draw_grad_out(key, part):
    key_noise = jax.random.fold_in(key, 21)
    key_offset = jax.random.fold_in(key, 22)
    normal_draw = jnp.clip(jax.random.normal(key_noise, (HEIGHT, COLS, C), jnp.float32), -4.0, 4.0)
    offset = jax.random.uniform(key_offset, (HEIGHT, 1, C), jnp.float32, -1.0, 3.0)
    return (offset + normal_draw).astype(jnp.bfloat16)


def centred(own_key, shape, scale, limit, held_as=jnp.bfloat16):
    entries = scale * jax.random.normal(own_key, shape, jnp.float32)
    return jnp.clip(entries, min=-limit, max=limit).astype(held_as)


def setup_inputs(seed: int = 0, part: int = 0) -> dict:
    streams_of = jax.random.split(jax.random.key(seed), 6)
    part_splits = jax.random.split(jax.random.fold_in(streams_of[5], part), 6)
    features = draw_features(jax.random.fold_in(jax.random.fold_in(streams_of[5], part), 71), part)
    grad_out = draw_grad_out(jax.random.fold_in(jax.random.fold_in(streams_of[5], part), 71), part)
    filters = centred(streams_of[2], (C, 3, 3, C), (9 * C) ** -0.5, 0.09375)
    norm_gain = jnp.clip(1.0 + 0.15 * jax.random.normal(streams_of[3], (C,), jnp.float32), 0.25, 1.75)
    norm_bias = jnp.clip(jax.random.uniform(streams_of[4], (C,), jnp.float32, -1.0, 1.0), -1.0, 1.0)
    return dict(features=features, grad_out=grad_out, filters=filters, norm_gain=norm_gain, norm_bias=norm_bias)


epsilon = 1e-06

def expand(values, channels):
    groups = values.shape[0]
    return jnp.broadcast_to(values[:, None], (groups, channels // groups)).reshape(channels)

def group_total(values):
    return values.reshape(GROUPS, -1).sum(axis=1)

def reference(features, grad_out, filters, norm_gain, norm_bias):
    height, columns, channels = features.shape
    pixels = height * columns
    members = pixels * (channels // GROUPS)
    widened = features.astype(jnp.float32)
    group_mean = group_total(lax.optimization_barrier(jnp.sum(widened, axis=(0, 1)))) / members
    centered = widened - expand(group_mean, channels)
    group_var = group_total(lax.optimization_barrier(jnp.sum(centered * centered, axis=(0, 1)))) / members
    inv_std = lax.rsqrt(group_var + epsilon)
    normalized = centered * expand(inv_std, channels)
    normed = normalized * norm_gain + norm_bias
    sigmoid_z = jax.nn.sigmoid(normed)
    activation = (normed * sigmoid_z).astype(jnp.bfloat16)
    flat_act = activation.reshape(-1, channels)
    padded = jnp.pad(grad_out, ((1, 1), (1, 1), (0, 0)))
    grad_act = jnp.zeros((pixels, channels), jnp.float32)
    pieces = []
    for tap_row in range(3):
        for tap_col in range(3):
            window = padded[2 - tap_row:2 - tap_row + height, 2 - tap_col:2 - tap_col + columns].reshape(-1, channels)
            grad_act = grad_act + jnp.dot(window, filters[:, tap_row, tap_col, :], preferred_element_type=jnp.float32)
            pieces.append(lax.dot_general(window, flat_act, (((0,), (0,)), ((), ())), preferred_element_type=jnp.float32))
    filter_grad = jnp.stack(pieces, axis=1).reshape(channels, 3, 3, channels) / pixels
    grad_pre = grad_act.reshape(height, columns, channels) * (sigmoid_z * (1.0 + normed * (1.0 - sigmoid_z)))
    bias_grad = lax.optimization_barrier(jnp.sum(grad_pre, axis=(0, 1)))
    gain_grad = lax.optimization_barrier(jnp.sum(grad_pre * normalized, axis=(0, 1)))
    mean_grad = group_total(norm_gain * bias_grad) / members
    mean_cross = group_total(norm_gain * gain_grad) / members
    grad_in = expand(inv_std, channels) * (grad_pre * norm_gain - expand(mean_grad, channels) - normalized * expand(mean_cross, channels))
    return (grad_in.astype(jnp.bfloat16), filter_grad, gain_grad, bias_grad)
```

```python
import functools
import math

import jax
import jax.numpy as jnp
from jax import lax
from jax.experimental import pallas as pl
from jax.experimental.pallas import tpu as pltpu
from jax.sharding import PartitionSpec as P

GROUPS = 32
LANES = 128
POWER = 9
TAPS = 9
LAG_B = 2
MAIN = 40
EPSILON = 1e-06
GAIN_MAX = 1.75
BIAS_MAX = 1.0
MESH = pl.DeviceIdType.MESH
F32 = jnp.float32
BF16 = jnp.bfloat16


def encode(value):
    square = value * value
    fourth = square * square
    return (fourth * fourth * value).astype(BF16)


def decode(coded):
    wide = coded.astype(F32)
    root = jnp.exp2(jnp.log2(jnp.maximum(jnp.abs(wide), 1e-38)) * (1.0 / POWER))
    root = jnp.where(jnp.abs(wide) < 1e-37, 0.0, root)
    return jnp.where(wide < 0.0, -root, root)


def group_sum(row, per_group):
    value = jnp.broadcast_to(row, (8, LANES))
    lane = lax.broadcasted_iota(jnp.int32, (8, LANES), 1)
    step = 1
    while step < per_group:
        low = pltpu.roll(value, step, 1)
        high = pltpu.roll(value, LANES - step, 1)
        value = value + jnp.where((lane & step) != 0, low, high)
        step *= 2
    return value[0:1]


def kernel(
    n, height, width, channels,
    feat_hbm, gout_hbm, filt_hbm, gain_hbm, bias_hbm,
    gin_ref, fg_ref, sums_ref,
    feat, featc, gext, filt, gt, act, gact, part, sa, ra, sb, rb, sm, rm, sc, rc, hs, hr,
    gin_s, gin_r, stat, tops, sums, gain_ref, bias_ref,
    feat_sem, local_sem, push_send, push_recv, halo_send, halo_recv,
    stat_send, stat_recv, tops_send, tops_recv, sums_send, sums_recv,
    a_send, a_recv, b_send, b_recv, m_send, m_recv, c_send, c_recv, h_send, h_recv,
):
    me = lax.axis_index("rows")
    core, chip = lax.rem(me, 2), lax.div(me, 2)
    mate = me + 1 - 2 * core
    chips = n // 2
    bits = chips.bit_length() - 1
    bit = [lax.rem(lax.div(chip, 1 << j), 2) for j in range(bits)]
    across = [(2 << j) * (1 - 2 * bit[j]) for j in range(bits)]
    block = channels // n
    half = channels // 2
    chunks = channels // LANES
    mine = half // LANES
    per_group = channels // GROUPS
    slab = height * width
    tall = 2 * height
    area = 2 * slab
    pixels = slab * n
    members = pixels * per_group
    own = pl.multiple_of(core * slab, slab)
    other = pl.multiple_of((1 - core) * slab, slab)
    my_cols = pl.multiple_of(core * half, LANES)
    mate_cols = pl.multiple_of((1 - core) * half, LANES)

    def remote(src, dst, send, recv, target):
        return pltpu.make_async_remote_copy(
            src_ref=src, dst_ref=dst, send_sem=send, recv_sem=recv,
            device_id={"rows": target}, device_id_type=MESH,
        )

    def peer(k):
        return lax.rem(me + k, n)

    def rows_of(h):
        return pl.ds(pl.multiple_of(h * width, width), width)

    in_feat = [
        pltpu.make_async_copy(
            feat_hbm.at[pl.ds(h * width, width)], feat.at[pl.ds(h * width, width)], feat_sem.at[h]
        )
        for h in range(height)
    ]
    in_gout = pltpu.make_async_copy(
        gout_hbm, gext.at[pl.ds(width + own, slab)], local_sem.at[0]
    )
    in_half = pltpu.make_async_copy(
        feat_hbm.at[:, pl.ds(my_cols, half)], featc.at[pl.ds(own, slab)], local_sem.at[1]
    )
    in_filt = pltpu.make_async_copy(
        filt_hbm.at[:, :, pl.ds(my_cols, half)], filt, local_sem.at[2]
    )
    in_gain = pltpu.make_async_copy(gain_hbm, gain_ref, local_sem.at[3])
    in_bias = pltpu.make_async_copy(bias_hbm, bias_ref, local_sem.at[4])
    for copy in in_feat:
        copy.start()
    in_gout.start()
    in_half.start()
    in_filt.start()
    in_gain.start()
    in_bias.start()

    barrier = pltpu.get_barrier_semaphore()

    def greet(k, carry):
        pl.semaphore_signal(barrier, inc=1, device_id={"rows": peer(k)}, device_id_type=MESH)
        return carry

    lax.fori_loop(1, n, greet, 0)

    def shared(buffer, send, recv):
        def copy(k, source):
            return remote(buffer.at[me], buffer.at[source], send.at[k], recv.at[source], peer(k))

        def start():
            def body(k, carry):
                copy(k, me).start()
                return carry
            lax.fori_loop(1, n, body, 0)

        def wait():
            def body(k, carry):
                copy(k, peer(k)).wait_recv()
                return carry
            lax.fori_loop(1, n, body, 0)

        def drain():
            def body(k, carry):
                copy(k, me).wait_send()
                return carry
            lax.fori_loop(1, n, body, 0)

        return start, wait, drain

    stat_start, stat_wait, stat_drain = shared(stat, stat_send, stat_recv)
    tops_start, tops_wait, tops_drain = shared(tops, tops_send, tops_recv)
    sums_start, sums_wait, sums_drain = shared(sums, sums_send, sums_recv)

    lane = lax.broadcasted_iota(jnp.int32, (1, LANES), 1)
    slot = lane & (per_group - 1)
    totals = [jnp.zeros((8, LANES), F32) for _ in range(chunks)]
    squares = [jnp.zeros((8, LANES), F32) for _ in range(chunks)]
    for h in range(height):
        in_feat[h].wait()
        for c in range(chunks):
            x = feat[h * width:(h + 1) * width, c * LANES:(c + 1) * LANES].astype(F32)
            x = x.reshape(width // 8, 8, LANES)
            totals[c] = totals[c] + x.sum(0)
            squares[c] = squares[c] + (x * x).sum(0)
    packed = jnp.zeros((1, LANES), F32)
    for c in range(chunks):
        total = group_sum(totals[c].sum(0, keepdims=True), per_group)
        square = group_sum(squares[c].sum(0, keepdims=True), per_group)
        packed = packed + jnp.where(slot == c, total, 0.0)
        packed = packed + jnp.where(slot == chunks + c, square, 0.0)
    stat[me] = packed

    pl.semaphore_wait(barrier, n - 1)
    stat_start()

    push_feat = remote(
        feat.at[:, pl.ds(mate_cols, half)], featc.at[pl.ds(own, slab)],
        push_send.at[0], push_recv.at[0], mate,
    )
    push_gout = remote(
        gext.at[pl.ds(width + own, slab)], gext.at[pl.ds(width + own, slab)],
        push_send.at[1], push_recv.at[1], mate,
    )
    push_feat.start()
    in_gout.wait()
    push_gout.start()

    above, below = pl.ds(0, width), pl.ds((tall + 1) * width, width)
    first, last = pl.ds(width, width), pl.ds(tall * width, width)

    def to_above(k):
        return remote(gext.at[first], gext.at[below], halo_send.at[k], halo_recv.at[0], me - 1 - k)

    def to_below(k):
        return remote(gext.at[last], gext.at[above], halo_send.at[k], halo_recv.at[1], me + 1 + k)

    has_above, has_below = chip > 0, chip < chips - 1

    @pl.when((core == 0) & has_above)
    def _():
        to_above(0).start()
        to_above(1).start()

    @pl.when((core == 1) & has_below)
    def _():
        to_below(0).start()
        to_below(1).start()

    @pl.when(chip == 0)
    def _():
        gext[above, :] = jnp.zeros((width, channels), BF16)

    @pl.when(chip == chips - 1)
    def _():
        gext[below, :] = jnp.zeros((width, channels), BF16)

    def top_step(h, carry):
        g = jnp.abs(gext[rows_of(1 + core * height + h), :])
        return jnp.maximum(carry, g.reshape(width // 16, 16, channels).max(0))

    largest = lax.fori_loop(0, height, top_step, jnp.zeros((16, channels), BF16))
    largest = largest.astype(F32).max(0, keepdims=True)
    top = jnp.zeros((1, LANES), F32)
    for c in range(chunks):
        top = jnp.maximum(top, largest[:, c * LANES:(c + 1) * LANES])
    tops[me] = top
    tops_start()

    column = lax.broadcasted_iota(jnp.int32, (width, LANES), 0)

    def from_left(x):
        return jnp.where(column > 0, pltpu.roll(x, 1, 0), 0.0)

    def from_right(x):
        return jnp.where(column < width - 1, pltpu.roll(x, width - 1, 0), 0.0)

    def conv(j):
        first_row = lax.rem(core * height + 1 + 2 * j, tall)
        where = [first_row, lax.rem(first_row + 1, tall)]
        ys = [[], []]
        for s in range(3):
            for m in range(2):
                y = None
                for r in range(3):
                    d = jnp.dot(
                        gext[rows_of(where[m] - r + 2), :], filt[3 * r + s],
                        preferred_element_type=F32,
                    )
                    y = d if y is None else y + d
                ys[m].append(y)
        for m in range(2):
            for k in range(mine):
                sub = slice(k * LANES, (k + 1) * LANES)
                y = ys[m]
                gact[rows_of(where[m]), sub] = (
                    y[1][:, sub] + from_right(y[0][:, sub]) + from_left(y[2][:, sub])
                )

    def transpose(e):
        start = pl.multiple_of(e * width, width)
        gt[:, pl.ds(start, width)] = gext[pl.ds(start, width), :].T

    def transposes(base, count):
        def body(e, carry):
            transpose(base + e)
            return carry
        lax.fori_loop(0, count, body, 0)

    transposes(1 + core * height, height)
    in_filt.wait()
    if height >= 4:
        conv(0)

    push_gout_in = remote(
        gext.at[pl.ds(width + other, slab)], gext.at[pl.ds(width + other, slab)],
        push_send.at[1], push_recv.at[1], mate,
    )
    push_feat_in = remote(
        feat.at[:, pl.ds(mate_cols, half)], featc.at[pl.ds(other, slab)],
        push_send.at[0], push_recv.at[0], mate,
    )
    push_gout_in.wait_recv()
    transposes(1 + (1 - core) * height, height)

    @pl.when(has_below)
    def _():
        to_above(0).wait_recv()

    @pl.when(has_above)
    def _():
        to_below(0).wait_recv()

    transpose(0)
    transpose(tall + 1)
    if height < 4:
        conv(0)
    conv(1)
    in_half.wait()
    in_gain.wait()
    in_bias.wait()
    push_feat_in.wait_recv()

    stat_wait()
    total_stat = stat[...].sum(0)
    means, invs, gains, biases = [], [], [], []
    for k in range(mine):
        which = core * mine + k
        total = group_sum(jnp.where(slot == which, total_stat, 0.0), per_group)
        square = group_sum(jnp.where(slot == chunks + which, total_stat, 0.0), per_group)
        mean = total / members
        means.append(mean)
        invs.append(lax.rsqrt(square / members - mean * mean + EPSILON))
        at = pl.ds(pl.multiple_of(my_cols + k * LANES, LANES), LANES)
        gains.append(gain_ref[:, at])
        biases.append(bias_ref[:, at])

    def forward(rows, k):
        cols = slice(k * LANES, (k + 1) * LANES)
        normalized = (featc[rows, cols].astype(F32) - means[k]) * invs[k]
        normed = normalized * gains[k] + biases[k]
        return normalized, normed, 1.0 / (1.0 + jnp.exp(-normed))

    def activate(h, carry):
        rows = rows_of(h)
        for k in range(mine):
            _, normed, sig = forward(rows, k)
            act[1, rows, k * LANES:(k + 1) * LANES] = (normed * sig).astype(BF16)
        return carry

    lax.fori_loop(0, tall, activate, 0)

    tops_wait()
    gmax = jnp.max(tops[...].max(0), axis=1, keepdims=True)
    bound = GAIN_MAX * math.sqrt(float(pixels) * float(members)) + BIAS_MAX * pixels
    reach = bound * jnp.maximum(gmax, 1e-30) * (2.0 ** -13.9)
    scale = 1.0 / reach

    def shift(h, carry):
        rows = rows_of(h)
        for k in range(mine):
            cols = slice(k * LANES, (k + 1) * LANES)
            a = act[1, rows, cols].astype(F32)
            act[0, rows, cols] = from_left(a).astype(BF16)
            act[2, rows, cols] = from_right(a).astype(BF16)
        return carry

    def multiply(t):
        s = lax.rem(1 + 2 * lax.div(t, 3), 3)
        start = pl.multiple_of((2 - lax.rem(t, 3)) * width, LANES)
        for m in range(2):
            result = jnp.dot(
                gt[m * half:(m + 1) * half, pl.ds(start, area)], act[s],
                preferred_element_type=F32,
            )
            part[t, m * (chips // 2):(m + 1) * (chips // 2)] = result.reshape(
                chips // 2, 2 * block, half
            )

    def swapped(t, k):
        return (1 - lax.rem(t, 2)) * k

    def pair_delta(kind):
        return kind * across[1] + (1 - kind) * across[0]

    def copy_a(t, k):
        target = me + pair_delta(swapped(t, k))
        return remote(sa.at[t, k], ra.at[t, k], a_send.at[t, k], a_recv.at[t, k], target)

    def copy_b(t, k):
        target = me + pair_delta(1 - swapped(t, k))
        return remote(sb.at[t, k], rb.at[t, k], b_send.at[t, k], b_recv.at[t, k], target)

    def copy_m(t, k, j):
        at = pl.ds(chips // 4 - (chips >> j), chips >> (j + 1))
        return remote(
            sm.at[t, k, at], rm.at[t, k, at],
            m_send.at[t, k, j], m_recv.at[t, k, j], me + across[j],
        )

    def copy_c(t, k, way, source):
        target = lax.div(me + across[bits - 1], 2) * 2 + way
        return remote(
            sc.at[t, k, way], rc.at[t, k, source],
            c_send.at[t, k, way], c_recv.at[t, k, source], target,
        )

    def copy_h(t, k):
        return remote(hs.at[t, k], hr.at[t, k], h_send.at[t, k], h_recv.at[t, k], mate)

    def lanes_of(k):
        return slice(k * LANES, (k + 1) * LANES)

    def stage_a(t, k):
        kind = swapped(t, k)
        for w in range(chips // 2):
            u, v = w >> 1, w & 1
            dest = u * 4 + kind * (2 * (1 - bit[1]) + v) + (1 - kind) * (2 * v + 1 - bit[0])
            sa[t, k, w] = encode(part[t, dest, :, lanes_of(k)] * scale)
        copy_a(t, k).start()

    def stage_b(t, k):
        copy_a(t, k).wait_recv()
        kind = swapped(t, k)
        mine_bit = kind * bit[0] + (1 - kind) * bit[1]

        def value(u, v):
            dest = u * 4 + kind * (2 * bit[1] + v) + (1 - kind) * (2 * v + bit[0])
            return part[t, dest, :, lanes_of(k)] * scale + decode(ra[t, k, 2 * u + v])

        for u in range(chips // 4):
            sb[t, k, u] = encode(value(u, 1 - mine_bit))
        copy_b(t, k).start()
        for u in range(chips // 4):
            part[t, u * 4 + 2 * bit[1] + bit[0], :, lanes_of(k)] = value(u, mine_bit)

    def low(j):
        return lax.rem(chip, 1 << j)

    def received(t, k, j):
        if j == 2:
            copy_b(t, k).wait_recv()
            return rb, 0
        copy_m(t, k, j - 1).wait_recv()
        return rm, chips // 4 - (chips >> (j - 1))

    def stage_m(t, k, j):
        buffer, base = received(t, k, j)

        def value(r, side):
            coded = buffer[t, k, base + 2 * r + side]
            return part[t, (2 * r + side) * (1 << j) + low(j), :, lanes_of(k)] + decode(coded)

        for r in range(chips >> (j + 1)):
            sm[t, k, chips // 4 - (chips >> j) + r] = encode(value(r, 1 - bit[j]))
        copy_m(t, k, j).start()
        for r in range(chips >> (j + 1)):
            part[t, (2 * r + bit[j]) * (1 << j) + low(j), :, lanes_of(k)] = value(r, bit[j])

    def stage_c(t, k):
        j = bits - 1
        buffer, base = received(t, k, j)

        def value(side, rows):
            coded = buffer[t, k, base + side, rows]
            return part[t, side * (1 << j) + low(j), rows, lanes_of(k)] + decode(coded)

        for way in range(2):
            rows = slice(way * block, (way + 1) * block)
            sc[t, k, way] = encode(value(1 - bit[j], rows))
            copy_c(t, k, way, core).start()
        hs[t, k] = value(bit[j], pl.ds(pl.multiple_of((1 - core) * block, block), block))
        copy_h(t, k).start()
        rows = pl.ds(pl.multiple_of(core * block, block), block)
        part[t, chip, rows, lanes_of(k)] = value(bit[j], rows)

    def stage_d(t, k):
        tap = 3 * lax.rem(t, 3) + lax.rem(1 + 2 * lax.div(t, 3), 3)
        rows = pl.ds(pl.multiple_of(core * block, block), block)
        copy_c(t, k, core, core).wait_recv()
        total = part[t, chip, rows, lanes_of(k)]
        total = total + decode(rc[t, k, core])
        at = pl.ds(pl.multiple_of(my_cols + k * LANES, LANES), LANES)
        fg_ref[tap, :, at] = total * (reach / pixels)
        copy_h(t, k).wait_recv()
        copy_c(t, k, core, 1 - core).wait_recv()
        total = hr[t, k] + decode(rc[t, k, 1 - core])
        at = pl.ds(pl.multiple_of(mate_cols + k * LANES, LANES), LANES)
        fg_ref[tap, :, at] = total * (reach / pixels)

    def gradients():
        for k in range(mine):
            cols = lanes_of(k)

            def grad_step(h, carry):
                bias_sum, gain_sum = carry
                rows = rows_of(h)
                normalized, normed, sig = forward(rows, k)
                pre = gact[rows, cols] * (sig * (1.0 + normed * (1.0 - sig)))
                gact[rows, cols] = pre
                return (
                    bias_sum + pre.reshape(width // 8, 8, LANES).sum(0),
                    gain_sum + (pre * normalized).reshape(width // 8, 8, LANES).sum(0),
                )

            zero = jnp.zeros((8, LANES), F32)
            bias_sum, gain_sum = lax.fori_loop(0, tall, grad_step, (zero, zero))
            sums[me, k:k + 1, :] = bias_sum.sum(0, keepdims=True)
            sums[me, mine + k:mine + k + 1, :] = gain_sum.sum(0, keepdims=True)
        sums_start()

    push_gin = remote(gin_s, gin_r, push_send.at[2], push_recv.at[2], mate)

    def finish():
        sums_wait()
        everyone = sums[...].reshape(chips, 2, 2 * mine, LANES).sum(0)
        for c in range(2):
            for k in range(mine):
                sums_ref[c * mine + k:c * mine + k + 1, :] = everyone[c, k:k + 1]
                sums_ref[chunks + c * mine + k:chunks + c * mine + k + 1, :] = (
                    everyone[c, mine + k:mine + k + 1]
                )
        for side in (1, 0):
            base = (1 - core if side else core) * height
            for k in range(mine):
                mean_grad = group_sum(
                    gains[k] * sums_ref[pl.ds(core * mine + k, 1), :], per_group
                ) / members
                mean_cross = group_sum(
                    gains[k] * sums_ref[pl.ds(chunks + core * mine + k, 1), :], per_group
                ) / members
                at = pl.ds(pl.multiple_of(my_cols + k * LANES, LANES), LANES)

                def final_step(h, carry):
                    rows = rows_of(base + h)
                    cols = lanes_of(k)
                    normalized = (featc[rows, cols].astype(F32) - means[k]) * invs[k]
                    result = invs[k] * (gact[rows, cols] * gains[k] - mean_grad - normalized * mean_cross)
                    if side:
                        gin_s[rows_of(h), cols] = result.astype(BF16)
                    else:
                        gin_ref[rows_of(h), at] = result.astype(BF16)
                    return carry

                lax.fori_loop(0, height, final_step, 0)
            if side:
                push_gin.start()

    lag_d = LAG_B + bits - 1

    def run(t, carry):
        @pl.when(t < TAPS)
        def _():
            multiply(t)
            for k in range(mine):
                stage_a(t, k)

        @pl.when(t == 0)
        def _():
            lax.fori_loop(0, tall, shift, 0)

        @pl.when((t >= 1) & (t < height - 1))
        def _():
            conv(t + 1)

        @pl.when(t == 3)
        def _():
            gradients()

        @pl.when(t == 6)
        def _():
            finish()

        @pl.when((t >= LAG_B) & (t < TAPS + LAG_B))
        def _():
            for k in range(mine):
                stage_b(t - LAG_B, k)

        for j in range(2, bits - 1):
            @pl.when((t >= LAG_B + j - 1) & (t < TAPS + LAG_B + j - 1))
            def _():
                for k in range(mine):
                    stage_m(t - LAG_B - j + 1, k, j)

        @pl.when((t >= lag_d - 1) & (t < TAPS + lag_d - 1))
        def _():
            for k in range(mine):
                stage_c(t - lag_d + 1, k)

        @pl.when(t >= lag_d)
        def _():
            for k in range(mine):
                stage_d(t - lag_d, k)

        return carry

    lax.fori_loop(0, TAPS + lag_d, run, 0)

    push_gin.wait_recv()

    def collect(h, carry):
        gin_ref[rows_of(h), pl.ds(mate_cols, half)] = gin_r[rows_of(h), :]
        return carry

    lax.fori_loop(0, height, collect, 0)

    def drain(t, carry):
        for k in range(mine):
            copy_a(t, k).wait_send()
            copy_b(t, k).wait_send()
            for j in range(2, bits - 1):
                copy_m(t, k, j).wait_send()
            for way in range(2):
                copy_c(t, k, way, core).wait_send()
            copy_h(t, k).wait_send()
        return carry

    lax.fori_loop(0, TAPS, drain, 0)
    push_feat.wait_send()
    push_gout.wait_send()
    push_gin.wait_send()
    stat_drain()
    tops_drain()
    sums_drain()

    @pl.when((core == 0) & has_above)
    def _():
        to_above(0).wait_send()
        to_above(1).wait_send()

    @pl.when((core == 1) & has_below)
    def _():
        to_below(0).wait_send()
        to_below(1).wait_send()


def hand_over(gin, fg, sums, gin_out, fg_out, gain_out, bias_out, sem):
    first = pltpu.make_async_copy(gin, gin_out, sem.at[0])
    second = pltpu.make_async_copy(fg, fg_out, sem.at[1])
    first.start()
    second.start()
    chunks = sums.shape[0] // 2
    for c in range(chunks):
        cols = slice(c * LANES, (c + 1) * LANES)
        bias_out[:, cols] = sums[c:c + 1, :]
        gain_out[:, cols] = sums[chunks + c:chunks + c + 1, :]
    first.wait()
    second.wait()


def local(n, features, grad_out, filters, norm_gain, norm_bias):
    height, width, channels = features.shape
    slab = height * width
    area, half = 2 * slab, channels // 2
    block, chips, chunks = channels // n, n // 2, channels // LANES
    mine = chunks // 2
    by_tap = filters.transpose(1, 2, 0, 3).reshape(TAPS, channels, channels)
    dma = pltpu.SemaphoreType.DMA
    hbm, vmem = pl.BlockSpec(memory_space=pltpu.HBM), pl.BlockSpec(memory_space=pltpu.VMEM)
    lots = dma((TAPS, mine))
    bits, middle = chips.bit_length() - 1, max(1, chips // 4 - 2)
    grad_in, filter_grad, sums = pl.pallas_call(
        functools.partial(kernel, n, height, width, channels),
        out_shape=(
            jax.ShapeDtypeStruct((slab, channels), BF16),
            jax.ShapeDtypeStruct((TAPS, block, channels), F32),
            jax.ShapeDtypeStruct((2 * chunks, LANES), F32),
        ),
        in_specs=[hbm] * 5,
        out_specs=(vmem, vmem, vmem),
        scratch_shapes=[
            pltpu.VMEM((slab, channels), BF16),
            pltpu.VMEM((area, half), BF16),
            pltpu.VMEM((area + 2 * width, channels), BF16),
            pltpu.VMEM((TAPS, channels, half), BF16),
            pltpu.VMEM((channels, area + 2 * width), BF16),
            pltpu.VMEM((3, area, half), BF16),
            pltpu.VMEM((area, half), F32),
            pltpu.VMEM((TAPS, chips, 2 * block, half), F32),
            pltpu.VMEM((TAPS, mine, chips // 2, 2 * block, LANES), BF16),
            pltpu.VMEM((TAPS, mine, chips // 2, 2 * block, LANES), BF16),
            pltpu.VMEM((TAPS, mine, chips // 4, 2 * block, LANES), BF16),
            pltpu.VMEM((TAPS, mine, chips // 4, 2 * block, LANES), BF16),
            pltpu.VMEM((TAPS, mine, middle, 2 * block, LANES), BF16),
            pltpu.VMEM((TAPS, mine, middle, 2 * block, LANES), BF16),
            pltpu.VMEM((TAPS, mine, 2, block, LANES), BF16),
            pltpu.VMEM((TAPS, mine, 2, block, LANES), BF16),
            pltpu.VMEM((TAPS, mine, block, LANES), F32),
            pltpu.VMEM((TAPS, mine, block, LANES), F32),
            pltpu.VMEM((slab, half), BF16),
            pltpu.VMEM((slab, half), BF16),
            pltpu.VMEM((n, 1, LANES), F32),
            pltpu.VMEM((n, 1, LANES), F32),
            pltpu.VMEM((n, 2 * mine, LANES), F32),
            pltpu.VMEM((1, channels), F32),
            pltpu.VMEM((1, channels), F32),
            dma((height,)), dma((5,)), dma((3,)), dma((3,)), dma((2,)), dma((2,)),
            dma((n,)), dma((n,)), dma((n,)), dma((n,)), dma((n,)), dma((n,)),
            lots, lots, lots, lots, dma((TAPS, mine, bits)), dma((TAPS, mine, bits)), dma((TAPS, mine, 2)), dma((TAPS, mine, 2)), lots, lots,
        ],
        compiler_params=pltpu.CompilerParams(
            collective_id=0, has_side_effects=True, vmem_limit_bytes=MAIN * 1024 * 1024
        ),
        name="block_backward",
    )(
        *(
            pltpu.with_memory_space_constraint(x, pltpu.HBM)
            for x in (
                features.reshape(slab, channels), grad_out.reshape(slab, channels), by_tap,
                norm_gain.reshape(1, channels), norm_bias.reshape(1, channels),
            )
        ),
    )
    grad_in, filter_grad, gain_grad, bias_grad = pl.pallas_call(
        hand_over,
        out_shape=(
            jax.ShapeDtypeStruct((slab, channels), BF16),
            jax.ShapeDtypeStruct((TAPS, block, channels), F32),
            jax.ShapeDtypeStruct((1, channels), F32),
            jax.ShapeDtypeStruct((1, channels), F32),
        ),
        in_specs=[vmem, vmem, vmem],
        out_specs=(hbm, hbm, vmem, vmem),
        scratch_shapes=[dma((2,))],
        compiler_params=pltpu.CompilerParams(vmem_limit_bytes=8 * 1024 * 1024),
        name="hand_over",
    )(grad_in, filter_grad, sums)
    return (
        grad_in.reshape(height, width, channels),
        filter_grad.transpose(1, 0, 2).reshape(block, 3, 3, channels),
        gain_grad.reshape(channels),
        bias_grad.reshape(channels),
    )


def solution(mesh):
    slabs = P(("parts", "rows"), None, None)
    return jax.shard_map(
        functools.partial(local, mesh.shape["rows"]),
        mesh=mesh,
        in_specs=(slabs, slabs, P(), P(), P()),
        out_specs=(slabs, P(("parts", "rows"), None, None, None), P("parts"), P("parts")),
        check_vma=False,
    )
```

```python
import functools
import math

import jax
import jax.numpy as jnp
from jax import lax
from jax.experimental import pallas as pl
from jax.experimental.pallas import tpu as pltpu
from jax.sharding import PartitionSpec as P

GROUPS = 32
LANES = 128
POWER = 9
TAPS = 9
LAG_B = 2
GAP = 2
LAST = 2
MAIN = 40
EPSILON = 1e-06
GAIN_MAX = 1.75
BIAS_MAX = 1.0
MESH = pl.DeviceIdType.MESH
F32 = jnp.float32
BF16 = jnp.bfloat16


def encode(value):
    square = value * value
    fourth = square * square
    return (fourth * fourth * value).astype(BF16)


def decode(coded):
    wide = coded.astype(F32)
    root = jnp.exp2(jnp.log2(jnp.maximum(jnp.abs(wide), 1e-38)) * (1.0 / POWER))
    root = jnp.where(jnp.abs(wide) < 1e-37, 0.0, root)
    return jnp.where(wide < 0.0, -root, root)


def group_sum(row, per_group):
    value = jnp.broadcast_to(row, (8, LANES))
    lane = lax.broadcasted_iota(jnp.int32, (8, LANES), 1)
    step = 1
    while step < per_group:
        low = pltpu.roll(value, step, 1)
        high = pltpu.roll(value, LANES - step, 1)
        value = value + jnp.where((lane & step) != 0, low, high)
        step *= 2
    return value[0:1]


def kernel(
    n, height, width, channels,
    feat_hbm, gout_hbm, filt_hbm, gain_hbm, bias_hbm,
    gin_ref, fg_ref, sums_ref,
    feat, featc, gext, filt, gt, act, gact, part, sa, ra, sb, rb, sm, rm, sc, rc, hs, hr, both,
    gin_s, gin_r, stat, tops, sums, gain_ref, bias_ref,
    feat_sem, local_sem, push_send, push_recv, halo_send, halo_recv,
    share_send, share_recv,
    out_send, a_recv, b_recv, m_recv, c_recv,
):
    me = lax.axis_index("rows")
    core, chip = lax.rem(me, 2), lax.div(me, 2)
    mate = me + 1 - 2 * core
    chips = n // 2
    bits = chips.bit_length() - 1
    bit = [lax.rem(lax.div(chip, 1 << j), 2) for j in range(bits)]
    across = [(2 << j) * (1 - 2 * bit[j]) for j in range(bits)]
    block = channels // n
    half = channels // 2
    chunks = channels // LANES
    mine = half // LANES
    per_group = channels // GROUPS
    slab = height * width
    tall = 2 * height
    area = 2 * slab
    pixels = slab * n
    members = pixels * per_group
    own = pl.multiple_of(core * slab, slab)
    other = pl.multiple_of((1 - core) * slab, slab)
    my_cols = pl.multiple_of(core * half, LANES)
    mate_cols = pl.multiple_of((1 - core) * half, LANES)

    def remote(src, dst, send, recv, target):
        return pltpu.make_async_remote_copy(
            src_ref=src, dst_ref=dst, send_sem=send, recv_sem=recv,
            device_id={"rows": target}, device_id_type=MESH,
        )

    def peer(k):
        return lax.rem(me + k, n)

    def rows_of(h):
        return pl.ds(pl.multiple_of(h * width, width), width)

    in_feat = [
        pltpu.make_async_copy(
            feat_hbm.at[pl.ds(h * width, width)], feat.at[pl.ds(h * width, width)], feat_sem.at[h]
        )
        for h in range(height)
    ]
    in_gout = pltpu.make_async_copy(
        gout_hbm, gext.at[pl.ds(width + own, slab)], local_sem.at[0]
    )
    in_half = pltpu.make_async_copy(
        feat_hbm.at[:, pl.ds(my_cols, half)], featc.at[pl.ds(own, slab)], local_sem.at[1]
    )
    in_filt = pltpu.make_async_copy(
        filt_hbm.at[:, :, pl.ds(my_cols, half)], filt, local_sem.at[2]
    )
    in_gain = pltpu.make_async_copy(gain_hbm, gain_ref, local_sem.at[3])
    in_bias = pltpu.make_async_copy(bias_hbm, bias_ref, local_sem.at[4])
    for copy in in_feat:
        copy.start()
    in_gout.start()

    barrier = pltpu.get_barrier_semaphore()

    def greet(k, carry):
        pl.semaphore_signal(barrier, inc=1, device_id={"rows": peer(k)}, device_id_type=MESH)
        return carry

    lax.fori_loop(1, n, greet, 0)

    def shared(buffer, j):
        def copy(k):
            return remote(
                buffer.at[me], buffer.at[me], share_send.at[j], share_recv.at[j], peer(k)
            )

        def start():
            def body(k, carry):
                copy(k).start()
                return carry
            lax.fori_loop(1, n, body, 0)

        others = buffer.at[pl.ds(0, n - 1)]
        every = remote(others, others, share_send.at[j], share_recv.at[j], mate)
        return start, every.wait_recv, every.wait_send

    stat_start, stat_wait, stat_drain = shared(stat, 0)
    tops_start, tops_wait, tops_drain = shared(tops, 1)
    sums_start, sums_wait, sums_drain = shared(sums, 2)

    lane = lax.broadcasted_iota(jnp.int32, (1, LANES), 1)
    slot = lane & (per_group - 1)
    totals = [jnp.zeros((8, LANES), F32) for _ in range(chunks)]
    squares = [jnp.zeros((8, LANES), F32) for _ in range(chunks)]
    for h in range(height):
        in_feat[h].wait()
        for c in range(chunks):
            x = feat[h * width:(h + 1) * width, c * LANES:(c + 1) * LANES].astype(F32)
            x = x.reshape(width // 8, 8, LANES)
            totals[c] = totals[c] + x.sum(0)
            squares[c] = squares[c] + (x * x).sum(0)
    packed = jnp.zeros((1, LANES), F32)
    for c in range(chunks):
        total = group_sum(totals[c].sum(0, keepdims=True), per_group)
        square = group_sum(squares[c].sum(0, keepdims=True), per_group)
        packed = packed + jnp.where(slot == c, total, 0.0)
        packed = packed + jnp.where(slot == chunks + c, square, 0.0)
    stat[me] = packed

    pl.semaphore_wait(barrier, n - 1)
    stat_start()

    push_feat = remote(
        feat.at[:, pl.ds(mate_cols, half)], featc.at[pl.ds(own, slab)],
        push_send.at[0], push_recv.at[0], mate,
    )
    push_gout = remote(
        gext.at[pl.ds(width + own, slab)], gext.at[pl.ds(width + own, slab)],
        push_send.at[1], push_recv.at[1], mate,
    )
    above, below = pl.ds(0, width), pl.ds((tall + 1) * width, width)
    first, last = pl.ds(width, width), pl.ds(tall * width, width)

    to_above = remote(gext.at[first], gext.at[below], halo_send.at[0], halo_recv.at[0], me - 1)
    to_below = remote(gext.at[last], gext.at[above], halo_send.at[0], halo_recv.at[0], me + 1)
    pass_above = remote(gext.at[above], gext.at[above], halo_send.at[1], halo_recv.at[1], mate)
    pass_below = remote(gext.at[below], gext.at[below], halo_send.at[1], halo_recv.at[1], mate)
    has_above, has_below = chip > 0, chip < chips - 1

    @pl.when(chip == 0)
    def _():
        gext[above, :] = jnp.zeros((width, channels), BF16)

    @pl.when(chip == chips - 1)
    def _():
        gext[below, :] = jnp.zeros((width, channels), BF16)

    in_gout.wait()

    def top_step(h, carry):
        g = jnp.abs(gext[rows_of(1 + core * height + h), :])
        return jnp.maximum(carry, g.reshape(width // 16, 16, channels).max(0))

    largest = lax.fori_loop(0, height, top_step, jnp.zeros((16, channels), BF16))
    largest = largest.astype(F32).max(0, keepdims=True)
    top = jnp.zeros((1, LANES), F32)
    for c in range(chunks):
        top = jnp.maximum(top, largest[:, c * LANES:(c + 1) * LANES])
    tops[me] = top
    tops_start()
    push_feat.start()
    push_gout.start()

    @pl.when((core == 0) & has_above)
    def _():
        to_above.start()

    @pl.when((core == 1) & has_below)
    def _():
        to_below.start()

    in_half.start()
    in_filt.start()
    in_gain.start()
    in_bias.start()

    column = lax.broadcasted_iota(jnp.int32, (width, LANES), 0)

    def from_left(x):
        return jnp.where(column > 0, pltpu.roll(x, 1, 0), 0.0)

    def from_right(x):
        return jnp.where(column < width - 1, pltpu.roll(x, width - 1, 0), 0.0)

    def conv(j):
        turned = core * (height - 2 - 2 * j) + j
        inner = lax.div(height - 1 - j + tall - 3, tall - 2)
        first_row = 1 + 2 * (inner * turned + (1 - inner) * j)
        where = [first_row, lax.rem(first_row + 1, tall)]
        ys = [[], []]
        for s in range(3):
            for m in range(2):
                y = None
                for r in range(3):
                    d = jnp.dot(
                        gext[rows_of(where[m] - r + 2), :], filt[3 * r + s],
                        preferred_element_type=F32,
                    )
                    y = d if y is None else y + d
                ys[m].append(y)
        for m in range(2):
            for k in range(mine):
                sub = slice(k * LANES, (k + 1) * LANES)
                y = ys[m]
                gact[rows_of(where[m]), sub] = (
                    y[1][:, sub] + from_right(y[0][:, sub]) + from_left(y[2][:, sub])
                )

    def transpose(e):
        start = pl.multiple_of(e * width, width)
        gt[:, pl.ds(start, width)] = gext[pl.ds(start, width), :].T

    def transposes(base, count):
        def body(e, carry):
            transpose(base + e)
            return carry
        lax.fori_loop(0, count, body, 0)

    transposes(1 + core * height, height)
    in_filt.wait()
    conv(0)

    push_gout_in = remote(
        gext.at[pl.ds(width + other, slab)], gext.at[pl.ds(width + other, slab)],
        push_send.at[1], push_recv.at[1], mate,
    )
    push_feat_in = remote(
        feat.at[:, pl.ds(mate_cols, half)], featc.at[pl.ds(other, slab)],
        push_send.at[0], push_recv.at[0], mate,
    )
    push_gout_in.wait_recv()
    transposes(1 + (1 - core) * height, height)

    in_half.wait()
    in_gain.wait()
    in_bias.wait()
    push_feat_in.wait_recv()

    stat_wait()
    total_stat = stat[...].sum(0)
    means, invs, gains, biases = [], [], [], []
    for k in range(mine):
        which = core * mine + k
        total = group_sum(jnp.where(slot == which, total_stat, 0.0), per_group)
        square = group_sum(jnp.where(slot == chunks + which, total_stat, 0.0), per_group)
        mean = total / members
        means.append(mean)
        invs.append(lax.rsqrt(square / members - mean * mean + EPSILON))
        at = pl.ds(pl.multiple_of(my_cols + k * LANES, LANES), LANES)
        gains.append(gain_ref[:, at])
        biases.append(bias_ref[:, at])

    def forward(rows, k):
        cols = slice(k * LANES, (k + 1) * LANES)
        normalized = (featc[rows, cols].astype(F32) - means[k]) * invs[k]
        normed = normalized * gains[k] + biases[k]
        return normalized, normed, 1.0 / (1.0 + jnp.exp(-normed))

    def activate(h, carry):
        rows = rows_of(h)
        for k in range(mine):
            _, normed, sig = forward(rows, k)
            act[1, rows, k * LANES:(k + 1) * LANES] = (normed * sig).astype(BF16)
        return carry

    lax.fori_loop(0, tall, activate, 0)

    tops_wait()
    gmax = jnp.max(tops[...].max(0), axis=1, keepdims=True)
    bound = GAIN_MAX * math.sqrt(float(pixels) * float(members)) + BIAS_MAX * pixels
    reach = bound * jnp.maximum(gmax, 1e-30) * (2.0 ** -13.9)
    scale = 1.0 / reach

    def shift(h, carry):
        rows = rows_of(h)
        for k in range(mine):
            cols = slice(k * LANES, (k + 1) * LANES)
            a = act[1, rows, cols].astype(F32)
            act[0, rows, cols] = from_left(a).astype(BF16)
            act[2, rows, cols] = from_right(a).astype(BF16)
        return carry

    def multiply(t):
        s = lax.rem(1 + 2 * lax.rem(t, 3), 3)
        r = lax.rem(1 + 2 * lax.div(t, 3), 3)
        start = pl.multiple_of((2 - r) * width, LANES)
        for m in range(2):
            result = jnp.dot(
                gt[m * half:(m + 1) * half, pl.ds(start, area)], act[s],
                preferred_element_type=F32,
            )
            part[t, m * (chips // 2):(m + 1) * (chips // 2)] = result.reshape(
                chips // 2, 2 * block, half
            )

    def swapped(t, k):
        return (1 - lax.rem(t, 2)) * k

    def pair_delta(kind):
        return kind * across[1] + (1 - kind) * across[0]

    def copy_a(t, k):
        target = me + pair_delta(swapped(t, k))
        return remote(sa.at[t, k], ra.at[t, k], out_send.at[0], a_recv.at[t, k], target)

    def copy_b(t, k):
        target = me + pair_delta(1 - swapped(t, k))
        return remote(sb.at[t, k], rb.at[t, k], out_send.at[1], b_recv.at[t, k], target)

    def copy_m(t, k, j):
        at = pl.ds(chips // 4 - (chips >> j), chips >> (j + 1))
        return remote(
            sm.at[t, k, at], rm.at[t, k, at],
            out_send.at[2], m_recv.at[t, k, j - 2], me + across[j],
        )

    def copy_c(t, k, way, source):
        target = lax.div(me + across[bits - 1], 2) * 2 + way
        return remote(
            sc.at[t, k, way], rc.at[t, k, source],
            out_send.at[3], c_recv.at[t, k], target,
        )

    def copy_h(t, k):
        return remote(hs.at[t, k], hr.at[t, k], out_send.at[4], c_recv.at[t, k], mate)

    def lanes_of(k):
        return slice(k * LANES, (k + 1) * LANES)

    def stage_a(t, k):
        kind = swapped(t, k)
        for w in range(chips // 2):
            u, v = w >> 1, w & 1
            dest = u * 4 + kind * (2 * (1 - bit[1]) + v) + (1 - kind) * (2 * v + 1 - bit[0])
            sa[t, k, w] = encode(part[t, dest, :, lanes_of(k)] * scale)
        copy_a(t, k).start()

    def stage_b(t, k):
        copy_a(t, k).wait_recv()
        kind = swapped(t, k)
        mine_bit = kind * bit[0] + (1 - kind) * bit[1]

        def value(u, v):
            dest = u * 4 + kind * (2 * bit[1] + v) + (1 - kind) * (2 * v + bit[0])
            return part[t, dest, :, lanes_of(k)] * scale + decode(ra[t, k, 2 * u + v])

        for u in range(chips // 4):
            sb[t, k, u] = encode(value(u, 1 - mine_bit))
        copy_b(t, k).start()
        for u in range(chips // 4):
            part[t, u * 4 + 2 * bit[1] + bit[0], :, lanes_of(k)] = value(u, mine_bit)

    def low(j):
        return lax.rem(chip, 1 << j)

    def received(t, k, j):
        if j == 2:
            copy_b(t, k).wait_recv()
            return rb, 0
        copy_m(t, k, j - 1).wait_recv()
        return rm, chips // 4 - (chips >> (j - 1))

    def stage_m(t, k, j):
        buffer, base = received(t, k, j)

        def value(r, side):
            coded = buffer[t, k, base + 2 * r + side]
            return part[t, (2 * r + side) * (1 << j) + low(j), :, lanes_of(k)] + decode(coded)

        for r in range(chips >> (j + 1)):
            sm[t, k, chips // 4 - (chips >> j) + r] = encode(value(r, 1 - bit[j]))
        copy_m(t, k, j).start()
        for r in range(chips >> (j + 1)):
            part[t, (2 * r + bit[j]) * (1 << j) + low(j), :, lanes_of(k)] = value(r, bit[j])

    def stage_c(t, k):
        j = bits - 1
        buffer, base = received(t, k, j)

        def value(side, rows):
            coded = buffer[t, k, base + side, rows]
            return part[t, side * (1 << j) + low(j), rows, lanes_of(k)] + decode(coded)

        for way in range(2):
            rows = slice(way * block, (way + 1) * block)
            sc[t, k, way] = encode(value(1 - bit[j], rows))
            copy_c(t, k, way, core).start()
        hs[t, k] = value(bit[j], pl.ds(pl.multiple_of((1 - core) * block, block), block))
        copy_h(t, k).start()
        rows = pl.ds(pl.multiple_of(core * block, block), block)
        part[t, chip, rows, lanes_of(k)] = value(bit[j], rows)

    def stage_d(t, k):
        tap = 3 * lax.rem(1 + 2 * lax.div(t, 3), 3) + lax.rem(1 + 2 * lax.rem(t, 3), 3)
        rows = pl.ds(pl.multiple_of(core * block, block), block)
        remote(both, both, out_send.at[3], c_recv.at[t, k], mate).wait_recv()
        total = part[t, chip, rows, lanes_of(k)]
        total = total + decode(rc[t, k, core])
        at = pl.ds(pl.multiple_of(my_cols + k * LANES, LANES), LANES)
        fg_ref[tap, :, at] = total * (reach / pixels)
        total = hr[t, k] + decode(rc[t, k, 1 - core])
        at = pl.ds(pl.multiple_of(mate_cols + k * LANES, LANES), LANES)
        fg_ref[tap, :, at] = total * (reach / pixels)

    def gradients():
        for k in range(mine):
            cols = lanes_of(k)

            def grad_step(h, carry):
                bias_sum, gain_sum = carry
                rows = rows_of(h)
                normalized, normed, sig = forward(rows, k)
                pre = gact[rows, cols] * (sig * (1.0 + normed * (1.0 - sig)))
                gact[rows, cols] = pre
                return (
                    bias_sum + pre.reshape(width // 8, 8, LANES).sum(0),
                    gain_sum + (pre * normalized).reshape(width // 8, 8, LANES).sum(0),
                )

            zero = jnp.zeros((8, LANES), F32)
            bias_sum, gain_sum = lax.fori_loop(0, tall, grad_step, (zero, zero))
            sums[me, k:k + 1, :] = bias_sum.sum(0, keepdims=True)
            sums[me, mine + k:mine + k + 1, :] = gain_sum.sum(0, keepdims=True)
        sums_start()

    push_gin = remote(gin_s, gin_r, push_send.at[2], push_recv.at[2], mate)

    def finish():
        sums_wait()
        everyone = sums[...].reshape(chips, 2, 2 * mine, LANES).sum(0)
        for c in range(2):
            for k in range(mine):
                sums_ref[c * mine + k:c * mine + k + 1, :] = everyone[c, k:k + 1]
                sums_ref[chunks + c * mine + k:chunks + c * mine + k + 1, :] = (
                    everyone[c, mine + k:mine + k + 1]
                )
        for side in (1, 0):
            base = (1 - core if side else core) * height
            for k in range(mine):
                mean_grad = group_sum(
                    gains[k] * sums_ref[pl.ds(core * mine + k, 1), :], per_group
                ) / members
                mean_cross = group_sum(
                    gains[k] * sums_ref[pl.ds(chunks + core * mine + k, 1), :], per_group
                ) / members
                at = pl.ds(pl.multiple_of(my_cols + k * LANES, LANES), LANES)

                def final_step(h, carry):
                    rows = rows_of(base + h)
                    cols = lanes_of(k)
                    normalized = (featc[rows, cols].astype(F32) - means[k]) * invs[k]
                    result = invs[k] * (gact[rows, cols] * gains[k] - mean_grad - normalized * mean_cross)
                    if side:
                        gin_s[rows_of(h), cols] = result.astype(BF16)
                    else:
                        gin_ref[rows_of(h), at] = result.astype(BF16)
                    return carry

                lax.fori_loop(0, height, final_step, 0)
            if side:
                push_gin.start()

    lag_c = LAG_B + GAP * (bits - 2)
    lag_d = lag_c + LAST

    def run(t, carry):
        @pl.when(t < TAPS)
        def _():
            multiply(t)
            for k in range(mine):
                stage_a(t, k)

        @pl.when(t == 0)
        def _():
            lax.fori_loop(0, tall, shift, 0)

            @pl.when((core == 0) & has_above)
            def _():
                to_below.wait_recv()
                pass_above.start()

            @pl.when((core == 1) & has_below)
            def _():
                to_above.wait_recv()
                pass_below.start()

        @pl.when(t == 2)
        def _():
            @pl.when((core == 1) & has_above)
            def _():
                pass_above.wait_recv()

            @pl.when((core == 0) & has_below)
            def _():
                pass_below.wait_recv()

            transpose(0)
            transpose(tall + 1)

        @pl.when((t >= 1) & (t < height))
        def _():
            conv(t)

        @pl.when(t == height)
        def _():
            gradients()

        @pl.when(t == 10)
        def _():
            finish()

        @pl.when((t >= LAG_B) & (t < TAPS + LAG_B))
        def _():
            for k in range(mine):
                stage_b(t - LAG_B, k)

        for j in range(2, bits - 1):
            lag_m = LAG_B + GAP * (j - 1)

            @pl.when((t >= lag_m) & (t < TAPS + lag_m))
            def _():
                for k in range(mine):
                    stage_m(t - lag_m, k, j)

        @pl.when((t >= lag_c) & (t < TAPS + lag_c))
        def _():
            for k in range(mine):
                stage_c(t - lag_c, k)

        @pl.when(t >= lag_d)
        def _():
            for k in range(mine):
                stage_d(t - lag_d, k)

        return carry

    lax.fori_loop(0, TAPS + lag_d, run, 0)

    push_gin.wait_recv()

    def collect(h, carry):
        gin_ref[rows_of(h), pl.ds(mate_cols, half)] = gin_r[rows_of(h), :]
        return carry

    lax.fori_loop(0, height, collect, 0)

    for j, (source, target) in enumerate(((sa, ra), (sb, rb), (sm, rm), (sc, rc), (hs, hr))):
        if j != 2 or bits > 3:
            remote(source, target, out_send.at[j], out_send.at[j], mate).wait_send()
    push_feat.wait_send()
    push_gout.wait_send()
    push_gin.wait_send()
    stat_drain()
    tops_drain()
    sums_drain()

    @pl.when((core == 0) & has_above)
    def _():
        to_above.wait_send()
        pass_above.wait_send()

    @pl.when((core == 1) & has_below)
    def _():
        to_below.wait_send()
        pass_below.wait_send()


def hand_over(gin, fg, sums, gin_out, fg_out, gain_out, bias_out, sem):
    first = pltpu.make_async_copy(gin, gin_out, sem.at[0])
    second = pltpu.make_async_copy(fg, fg_out, sem.at[1])
    first.start()
    second.start()
    chunks = sums.shape[0] // 2
    for c in range(chunks):
        cols = slice(c * LANES, (c + 1) * LANES)
        bias_out[:, cols] = sums[c:c + 1, :]
        gain_out[:, cols] = sums[chunks + c:chunks + c + 1, :]
    first.wait()
    second.wait()


def local(n, features, grad_out, filters, norm_gain, norm_bias):
    height, width, channels = features.shape
    slab = height * width
    area, half = 2 * slab, channels // 2
    block, chips, chunks = channels // n, n // 2, channels // LANES
    mine = chunks // 2
    by_tap = filters.transpose(1, 2, 0, 3).reshape(TAPS, channels, channels)
    dma = pltpu.SemaphoreType.DMA
    hbm, vmem = pl.BlockSpec(memory_space=pltpu.HBM), pl.BlockSpec(memory_space=pltpu.VMEM)
    lots = dma((TAPS, mine))
    bits, middle = chips.bit_length() - 1, max(1, chips // 4 - 2)
    grad_in, filter_grad, sums = pl.pallas_call(
        functools.partial(kernel, n, height, width, channels),
        out_shape=(
            jax.ShapeDtypeStruct((slab, channels), BF16),
            jax.ShapeDtypeStruct((TAPS, block, channels), F32),
            jax.ShapeDtypeStruct((2 * chunks, LANES), F32),
        ),
        in_specs=[hbm] * 5,
        out_specs=(vmem, vmem, vmem),
        scratch_shapes=[
            pltpu.VMEM((slab, channels), BF16),
            pltpu.VMEM((area, half), BF16),
            pltpu.VMEM((area + 2 * width, channels), BF16),
            pltpu.VMEM((TAPS, channels, half), BF16),
            pltpu.VMEM((channels, area + 2 * width), BF16),
            pltpu.VMEM((3, area, half), BF16),
            pltpu.VMEM((area, half), F32),
            pltpu.VMEM((TAPS, chips, 2 * block, half), F32),
            pltpu.VMEM((TAPS, mine, chips // 2, 2 * block, LANES), BF16),
            pltpu.VMEM((TAPS, mine, chips // 2, 2 * block, LANES), BF16),
            pltpu.VMEM((TAPS, mine, chips // 4, 2 * block, LANES), BF16),
            pltpu.VMEM((TAPS, mine, chips // 4, 2 * block, LANES), BF16),
            pltpu.VMEM((TAPS, mine, middle, 2 * block, LANES), BF16),
            pltpu.VMEM((TAPS, mine, middle, 2 * block, LANES), BF16),
            pltpu.VMEM((TAPS, mine, 2, block, LANES), BF16),
            pltpu.VMEM((TAPS, mine, 2, block, LANES), BF16),
            pltpu.VMEM((TAPS, mine, block, LANES), F32),
            pltpu.VMEM((TAPS, mine, block, LANES), F32),
            pltpu.VMEM((2, block, LANES), F32),
            pltpu.VMEM((slab, half), BF16),
            pltpu.VMEM((slab, half), BF16),
            pltpu.VMEM((n, 1, LANES), F32),
            pltpu.VMEM((n, 1, LANES), F32),
            pltpu.VMEM((n, 2 * mine, LANES), F32),
            pltpu.VMEM((1, channels), F32),
            pltpu.VMEM((1, channels), F32),
            dma((height,)), dma((5,)), dma((3,)), dma((3,)), dma((2,)), dma((2,)),
            dma((3,)), dma((3,)),
            dma((5,)), lots, lots, dma((TAPS, mine, middle)), lots,
        ],
        compiler_params=pltpu.CompilerParams(
            collective_id=0, has_side_effects=True, vmem_limit_bytes=MAIN * 1024 * 1024
        ),
        name="block_backward",
    )(
        *(
            pltpu.with_memory_space_constraint(x, pltpu.HBM)
            for x in (
                features.reshape(slab, channels), grad_out.reshape(slab, channels), by_tap,
                norm_gain.reshape(1, channels), norm_bias.reshape(1, channels),
            )
        ),
    )
    grad_in, filter_grad, gain_grad, bias_grad = pl.pallas_call(
        hand_over,
        out_shape=(
            jax.ShapeDtypeStruct((slab, channels), BF16),
            jax.ShapeDtypeStruct((TAPS, block, channels), F32),
            jax.ShapeDtypeStruct((1, channels), F32),
            jax.ShapeDtypeStruct((1, channels), F32),
        ),
        in_specs=[vmem, vmem, vmem],
        out_specs=(hbm, hbm, vmem, vmem),
        scratch_shapes=[dma((2,))],
        compiler_params=pltpu.CompilerParams(vmem_limit_bytes=8 * 1024 * 1024),
        name="hand_over",
    )(grad_in, filter_grad, sums)
    return (
        grad_in.reshape(height, width, channels),
        filter_grad.transpose(1, 0, 2).reshape(block, 3, 3, channels),
        gain_grad.reshape(channels),
        bias_grad.reshape(channels),
    )


def solution(mesh):
    slabs = P(("parts", "rows"), None, None)
    return jax.shard_map(
        functools.partial(local, mesh.shape["rows"]),
        mesh=mesh,
        in_specs=(slabs, slabs, P(), P(), P()),
        out_specs=(slabs, P(("parts", "rows"), None, None, None), P("parts"), P("parts")),
        check_vma=False,
    )
```

```python
import functools
import math

import jax
import jax.numpy as jnp
from jax import lax
from jax.experimental import pallas as pl
from jax.experimental.pallas import tpu as pltpu
from jax.sharding import PartitionSpec as P

GROUPS = 32
LANES = 128
POWER = 9
TAPS = 9
SWAPPED = 5
PLAN = (
    ("shift", "relay"), (), ("conv1", "edges"), ("b00",), ("b10",), ("b01", "conv2", "b20"),
    ("b30", "c00", "conv3", "b40", "c10"), ("grad", "b11", "b50", "c20", "b51"),
    ("b21", "b31", "b41", "c30", "c01", "c40"),
)
REST = (
    "b60", "b61", "c50", "c51", "b70", "c60", "d00", "b71", "c11", "c61", "d10", "d20",
    "b80", "c70", "fin1", "b81", "c71", "c21", "c31", "c80", "c41", "d30", "c81", "fin0", "d40",
    "d01", "d50", "d51", "d60", "d11", "d61", "d70", "d71", "d21", "d31", "d80", "d41", "d81",
)
MAIN = 40
EPSILON = 1e-06
GAIN_MAX = 1.75
BIAS_MAX = 1.0
MESH = pl.DeviceIdType.MESH
F32 = jnp.float32
BF16 = jnp.bfloat16


def encode(value):
    square = value * value
    fourth = square * square
    return (fourth * fourth * value).astype(BF16)


def decode(coded):
    wide = coded.astype(F32)
    root = jnp.exp2(jnp.log2(jnp.maximum(jnp.abs(wide), 1e-38)) * (1.0 / POWER))
    root = jnp.where(jnp.abs(wide) < 1e-37, 0.0, root)
    return jnp.where(wide < 0.0, -root, root)


def group_sum(row, per_group):
    value = jnp.broadcast_to(row, (8, LANES))
    lane = lax.broadcasted_iota(jnp.int32, (8, LANES), 1)
    step = 1
    while step < per_group:
        low = pltpu.roll(value, step, 1)
        high = pltpu.roll(value, LANES - step, 1)
        value = value + jnp.where((lane & step) != 0, low, high)
        step *= 2
    return value[0:1]


def kernel(
    n, height, width, channels,
    feat_hbm, gout_hbm, filt_hbm, gain_hbm, bias_hbm,
    gin_ref, fg_ref, sums_ref,
    feat, featc, gext, filt, gt, act, gact, part, sa, ra, sb, rb, sm, rm, sc, rc, hs, hr, both,
    gin_s, gin_r, stat, tops, sums, gain_ref, bias_ref,
    feat_sem, local_sem, push_send, push_recv, halo_send, halo_recv,
    share_send, share_recv,
    out_send, a_recv, b_recv, m_recv, c_recv,
):
    me = lax.axis_index("rows")
    core, chip = lax.rem(me, 2), lax.div(me, 2)
    mate = me + 1 - 2 * core
    chips = n // 2
    bits = chips.bit_length() - 1
    bit = [lax.rem(lax.div(chip, 1 << j), 2) for j in range(bits)]
    across = [(2 << j) * (1 - 2 * bit[j]) for j in range(bits)]
    block = channels // n
    half = channels // 2
    chunks = channels // LANES
    mine = half // LANES
    per_group = channels // GROUPS
    slab = height * width
    tall = 2 * height
    area = 2 * slab
    pixels = slab * n
    members = pixels * per_group
    own = pl.multiple_of(core * slab, slab)
    other = pl.multiple_of((1 - core) * slab, slab)
    my_cols = pl.multiple_of(core * half, LANES)
    mate_cols = pl.multiple_of((1 - core) * half, LANES)

    def remote(src, dst, send, recv, target):
        return pltpu.make_async_remote_copy(
            src_ref=src, dst_ref=dst, send_sem=send, recv_sem=recv,
            device_id={"rows": target}, device_id_type=MESH,
        )

    def peer(k):
        return lax.rem(me + k, n)

    def rows_of(h):
        return pl.ds(pl.multiple_of(h * width, width), width)

    in_feat = [
        pltpu.make_async_copy(
            feat_hbm.at[pl.ds(h * width, width)], feat.at[pl.ds(h * width, width)], feat_sem.at[h]
        )
        for h in range(height)
    ]
    in_gout = pltpu.make_async_copy(
        gout_hbm, gext.at[pl.ds(width + own, slab)], local_sem.at[0]
    )
    in_half = pltpu.make_async_copy(
        feat_hbm.at[:, pl.ds(my_cols, half)], featc.at[pl.ds(own, slab)], local_sem.at[1]
    )
    in_filt = pltpu.make_async_copy(
        filt_hbm.at[:, :, pl.ds(my_cols, half)], filt, local_sem.at[2]
    )
    in_gain = pltpu.make_async_copy(gain_hbm, gain_ref, local_sem.at[3])
    in_bias = pltpu.make_async_copy(bias_hbm, bias_ref, local_sem.at[4])
    for copy in in_feat:
        copy.start()

    barrier = pltpu.get_barrier_semaphore()

    def greet(k, carry):
        pl.semaphore_signal(barrier, inc=1, device_id={"rows": peer(k)}, device_id_type=MESH)
        return carry

    lax.fori_loop(1, n, greet, 0)

    in_gout.start()

    def shared(buffer, j):
        def copy(k):
            return remote(
                buffer.at[me], buffer.at[me], share_send.at[j], share_recv.at[j], peer(k)
            )

        def start():
            def body(k, carry):
                copy(k).start()
                return carry
            lax.fori_loop(1, n, body, 0)

        others = buffer.at[pl.ds(0, n - 1)]
        every = remote(others, others, share_send.at[j], share_recv.at[j], mate)
        return start, every.wait_recv, every.wait_send

    stat_start, stat_wait, stat_drain = shared(stat, 0)
    tops_start, tops_wait, tops_drain = shared(tops, 1)
    sums_start, sums_wait, sums_drain = shared(sums, 2)

    lane = lax.broadcasted_iota(jnp.int32, (1, LANES), 1)
    slot = lane & (per_group - 1)
    totals = [jnp.zeros((8, LANES), F32) for _ in range(chunks)]
    squares = [jnp.zeros((8, LANES), F32) for _ in range(chunks)]
    for h in range(height):
        in_feat[h].wait()
        for c in range(chunks):
            x = feat[h * width:(h + 1) * width, c * LANES:(c + 1) * LANES].astype(F32)
            x = x.reshape(width // 8, 8, LANES)
            totals[c] = totals[c] + x.sum(0)
            squares[c] = squares[c] + (x * x).sum(0)
    in_half.start()
    in_filt.start()
    in_gain.start()
    in_bias.start()
    packed = jnp.zeros((1, LANES), F32)
    for c in range(chunks):
        total = group_sum(totals[c].sum(0, keepdims=True), per_group)
        square = group_sum(squares[c].sum(0, keepdims=True), per_group)
        packed = packed + jnp.where(slot == c, total, 0.0)
        packed = packed + jnp.where(slot == chunks + c, square, 0.0)
    stat[me] = packed

    in_gout.wait()

    def top_step(h, carry):
        g = jnp.abs(gext[rows_of(1 + core * height + h), :])
        return jnp.maximum(carry, g.reshape(width // 16, 16, channels).max(0))

    largest = lax.fori_loop(0, height, top_step, jnp.zeros((16, channels), BF16))
    largest = largest.astype(F32).max(0, keepdims=True)
    top = jnp.zeros((1, LANES), F32)
    for c in range(chunks):
        top = jnp.maximum(top, largest[:, c * LANES:(c + 1) * LANES])
    tops[me] = top
    push_feat = remote(
        feat.at[:, pl.ds(mate_cols, half)], featc.at[pl.ds(own, slab)],
        push_send.at[0], push_recv.at[0], mate,
    )
    push_gout = remote(
        gext.at[pl.ds(width + own, slab)], gext.at[pl.ds(width + own, slab)],
        push_send.at[1], push_recv.at[1], mate,
    )
    pl.semaphore_wait(barrier, n - 1)
    stat_start()
    tops_start()
    push_gout.start()
    push_feat.start()

    above, below = pl.ds(0, width), pl.ds((tall + 1) * width, width)
    first, last = pl.ds(width, width), pl.ds(tall * width, width)

    to_above = remote(gext.at[first], gext.at[below], halo_send.at[0], halo_recv.at[0], me - 1)
    to_below = remote(gext.at[last], gext.at[above], halo_send.at[0], halo_recv.at[0], me + 1)
    pass_above = remote(gext.at[above], gext.at[above], halo_send.at[1], halo_recv.at[1], mate)
    pass_below = remote(gext.at[below], gext.at[below], halo_send.at[1], halo_recv.at[1], mate)
    has_above, has_below = chip > 0, chip < chips - 1

    @pl.when(chip == 0)
    def _():
        gext[above, :] = jnp.zeros((width, channels), BF16)

    @pl.when(chip == chips - 1)
    def _():
        gext[below, :] = jnp.zeros((width, channels), BF16)


    @pl.when((core == 0) & has_above)
    def _():
        to_above.start()

    @pl.when((core == 1) & has_below)
    def _():
        to_below.start()


    column = lax.broadcasted_iota(jnp.int32, (width, LANES), 0)

    def from_left(x):
        return jnp.where(column > 0, pltpu.roll(x, 1, 0), 0.0)

    def from_right(x):
        return jnp.where(column < width - 1, pltpu.roll(x, width - 1, 0), 0.0)

    def conv(j):
        turned = core * (height - 2 - 2 * j) + j
        inner = lax.div(height - 1 - j + tall - 3, tall - 2)
        first_row = 1 + 2 * (inner * turned + (1 - inner) * j)
        where = [first_row, lax.rem(first_row + 1, tall)]
        ys = [[], []]
        for s in range(3):
            for m in range(2):
                y = None
                for r in range(3):
                    d = jnp.dot(
                        gext[rows_of(where[m] - r + 2), :], filt[3 * r + s],
                        preferred_element_type=F32,
                    )
                    y = d if y is None else y + d
                ys[m].append(y)
        for m in range(2):
            for k in range(mine):
                sub = slice(k * LANES, (k + 1) * LANES)
                y = ys[m]
                gact[rows_of(where[m]), sub] = (
                    y[1][:, sub] + from_right(y[0][:, sub]) + from_left(y[2][:, sub])
                )

    def transpose(e):
        start = pl.multiple_of(e * width, width)
        gt[:, pl.ds(start, width)] = gext[pl.ds(start, width), :].T

    def transposes(base, count):
        def body(e, carry):
            transpose(base + e)
            return carry
        lax.fori_loop(0, count, body, 0)

    transposes(1 + core * height, height)
    in_filt.wait()
    conv(0)

    push_gout_in = remote(
        gext.at[pl.ds(width + other, slab)], gext.at[pl.ds(width + other, slab)],
        push_send.at[1], push_recv.at[1], mate,
    )
    push_feat_in = remote(
        feat.at[:, pl.ds(mate_cols, half)], featc.at[pl.ds(other, slab)],
        push_send.at[0], push_recv.at[0], mate,
    )
    push_gout_in.wait_recv()
    transposes(1 + (1 - core) * height, height)

    in_half.wait()
    in_gain.wait()
    in_bias.wait()
    push_feat_in.wait_recv()

    stat_wait()
    total_stat = stat[...].sum(0)
    means, invs, gains, biases = [], [], [], []
    for k in range(mine):
        which = core * mine + k
        total = group_sum(jnp.where(slot == which, total_stat, 0.0), per_group)
        square = group_sum(jnp.where(slot == chunks + which, total_stat, 0.0), per_group)
        mean = total / members
        means.append(mean)
        invs.append(lax.rsqrt(square / members - mean * mean + EPSILON))
        at = pl.ds(pl.multiple_of(my_cols + k * LANES, LANES), LANES)
        gains.append(gain_ref[:, at])
        biases.append(bias_ref[:, at])

    def forward(rows, k):
        cols = slice(k * LANES, (k + 1) * LANES)
        normalized = (featc[rows, cols].astype(F32) - means[k]) * invs[k]
        normed = normalized * gains[k] + biases[k]
        return normalized, normed, 1.0 / (1.0 + jnp.exp(-normed))

    def activate(h, carry):
        rows = rows_of(h)
        for k in range(mine):
            _, normed, sig = forward(rows, k)
            act[1, rows, k * LANES:(k + 1) * LANES] = (normed * sig).astype(BF16)
        return carry

    lax.fori_loop(0, tall, activate, 0)

    tops_wait()
    gmax = jnp.max(tops[...].max(0), axis=1, keepdims=True)
    bound = GAIN_MAX * math.sqrt(float(pixels) * float(members)) + BIAS_MAX * pixels
    reach = bound * jnp.maximum(gmax, 1e-30) * (2.0 ** -13.9)
    scale = 1.0 / reach

    def shift(h, carry):
        rows = rows_of(h)
        for k in range(mine):
            cols = slice(k * LANES, (k + 1) * LANES)
            a = act[1, rows, cols].astype(F32)
            act[0, rows, cols] = from_left(a).astype(BF16)
            act[2, rows, cols] = from_right(a).astype(BF16)
        return carry

    def multiply(t):
        s = lax.rem(1 + 2 * lax.rem(t, 3), 3)
        r = lax.rem(1 + 2 * lax.div(t, 3), 3)
        start = pl.multiple_of((2 - r) * width, LANES)
        for m in range(2):
            result = jnp.dot(
                gt[m * half:(m + 1) * half, pl.ds(start, area)], act[s],
                preferred_element_type=F32,
            )
            part[t, m * (chips // 2):(m + 1) * (chips // 2)] = result.reshape(
                chips // 2, 2 * block, half
            )

    def reached(t, least):
        return lax.div(t + TAPS - least, TAPS)

    def swapped(t, k):
        return k * (1 - reached(t, SWAPPED))

    def pair_delta(kind):
        return kind * across[1] + (1 - kind) * across[0]

    def copy_a(t, k):
        target = me + pair_delta(swapped(t, k))
        return remote(sa.at[t, k], ra.at[t, k], out_send.at[0], a_recv.at[t, k], target)

    def copy_b(t, k):
        target = me + pair_delta(1 - swapped(t, k))
        return remote(sb.at[t, k], rb.at[t, k], out_send.at[1], b_recv.at[t, k], target)

    def copy_m(t, k, j):
        at = pl.ds(chips // 4 - (chips >> j), chips >> (j + 1))
        return remote(
            sm.at[t, k, at], rm.at[t, k, at],
            out_send.at[2], m_recv.at[t, k, j - 2], me + across[j],
        )

    def copy_c(t, k, way, source):
        target = lax.div(me + across[bits - 1], 2) * 2 + way
        return remote(
            sc.at[t, k, way], rc.at[t, k, source],
            out_send.at[3], c_recv.at[t, k], target,
        )

    def copy_h(t, k):
        return remote(hs.at[t, k], hr.at[t, k], out_send.at[4], c_recv.at[t, k], mate)

    def lanes_of(k):
        return slice(k * LANES, (k + 1) * LANES)

    def stage_a(t, k):
        kind = swapped(t, k)
        for w in range(chips // 2):
            u, v = w >> 1, w & 1
            dest = u * 4 + kind * (2 * (1 - bit[1]) + v) + (1 - kind) * (2 * v + 1 - bit[0])
            sa[t, k, w] = encode(part[t, dest, :, lanes_of(k)] * scale)
        copy_a(t, k).start()

    def stage_b(t, k):
        copy_a(t, k).wait_recv()
        kind = swapped(t, k)
        mine_bit = kind * bit[0] + (1 - kind) * bit[1]

        def value(u, v):
            dest = u * 4 + kind * (2 * bit[1] + v) + (1 - kind) * (2 * v + bit[0])
            return part[t, dest, :, lanes_of(k)] * scale + decode(ra[t, k, 2 * u + v])

        for u in range(chips // 4):
            sb[t, k, u] = encode(value(u, 1 - mine_bit))
        copy_b(t, k).start()
        for u in range(chips // 4):
            part[t, u * 4 + 2 * bit[1] + bit[0], :, lanes_of(k)] = value(u, mine_bit)

    def low(j):
        return lax.rem(chip, 1 << j)

    def received(t, k, j):
        if j == 2:
            copy_b(t, k).wait_recv()
            return rb, 0
        copy_m(t, k, j - 1).wait_recv()
        return rm, chips // 4 - (chips >> (j - 1))

    def stage_m(t, k, j):
        buffer, base = received(t, k, j)

        def value(r, side):
            coded = buffer[t, k, base + 2 * r + side]
            return part[t, (2 * r + side) * (1 << j) + low(j), :, lanes_of(k)] + decode(coded)

        for r in range(chips >> (j + 1)):
            sm[t, k, chips // 4 - (chips >> j) + r] = encode(value(r, 1 - bit[j]))
        copy_m(t, k, j).start()
        for r in range(chips >> (j + 1)):
            part[t, (2 * r + bit[j]) * (1 << j) + low(j), :, lanes_of(k)] = value(r, bit[j])

    def stage_c(t, k):
        j = bits - 1
        buffer, base = received(t, k, j)

        def value(side, rows):
            coded = buffer[t, k, base + side, rows]
            return part[t, side * (1 << j) + low(j), rows, lanes_of(k)] + decode(coded)

        for way in range(2):
            rows = slice(way * block, (way + 1) * block)
            sc[t, k, way] = encode(value(1 - bit[j], rows))
            copy_c(t, k, way, core).start()
        hs[t, k] = value(bit[j], pl.ds(pl.multiple_of((1 - core) * block, block), block))
        copy_h(t, k).start()
        rows = pl.ds(pl.multiple_of(core * block, block), block)
        part[t, chip, rows, lanes_of(k)] = value(bit[j], rows)

    def stage_d(t, k):
        tap = 3 * lax.rem(1 + 2 * lax.div(t, 3), 3) + lax.rem(1 + 2 * lax.rem(t, 3), 3)
        rows = pl.ds(pl.multiple_of(core * block, block), block)
        remote(both, both, out_send.at[3], c_recv.at[t, k], mate).wait_recv()
        total = part[t, chip, rows, lanes_of(k)]
        total = total + decode(rc[t, k, core])
        at = pl.ds(pl.multiple_of(my_cols + k * LANES, LANES), LANES)
        fg_ref[tap, :, at] = total * (reach / pixels)
        total = hr[t, k] + decode(rc[t, k, 1 - core])
        at = pl.ds(pl.multiple_of(mate_cols + k * LANES, LANES), LANES)
        fg_ref[tap, :, at] = total * (reach / pixels)

    def gradients():
        for k in range(mine):
            cols = lanes_of(k)

            def grad_step(h, carry):
                bias_sum, gain_sum = carry
                rows = rows_of(h)
                normalized, normed, sig = forward(rows, k)
                pre = gact[rows, cols] * (sig * (1.0 + normed * (1.0 - sig)))
                gact[rows, cols] = pre
                return (
                    bias_sum + pre.reshape(width // 8, 8, LANES).sum(0),
                    gain_sum + (pre * normalized).reshape(width // 8, 8, LANES).sum(0),
                )

            zero = jnp.zeros((8, LANES), F32)
            bias_sum, gain_sum = lax.fori_loop(0, tall, grad_step, (zero, zero))
            sums[me, k:k + 1, :] = bias_sum.sum(0, keepdims=True)
            sums[me, mine + k:mine + k + 1, :] = gain_sum.sum(0, keepdims=True)
        sums_start()

    push_gin = remote(gin_s, gin_r, push_send.at[2], push_recv.at[2], mate)

    def finish():
        sums_wait()
        everyone = sums[...].reshape(chips, 2, 2 * mine, LANES).sum(0)
        for c in range(2):
            for k in range(mine):
                sums_ref[c * mine + k:c * mine + k + 1, :] = everyone[c, k:k + 1]
                sums_ref[chunks + c * mine + k:chunks + c * mine + k + 1, :] = (
                    everyone[c, mine + k:mine + k + 1]
                )
        half_finish(1)
        push_gin.start()

    def half_finish(side):
        base = (1 - core if side else core) * height
        for k in range(mine):
            mean_grad = group_sum(
                gains[k] * sums_ref[pl.ds(core * mine + k, 1), :], per_group
            ) / members
            mean_cross = group_sum(
                gains[k] * sums_ref[pl.ds(chunks + core * mine + k, 1), :], per_group
            ) / members
            at = pl.ds(pl.multiple_of(my_cols + k * LANES, LANES), LANES)

            def final_step(h, carry):
                rows = rows_of(base + h)
                cols = lanes_of(k)
                normalized = (featc[rows, cols].astype(F32) - means[k]) * invs[k]
                result = invs[k] * (gact[rows, cols] * gains[k] - mean_grad - normalized * mean_cross)
                if side:
                    gin_s[rows_of(h), cols] = result.astype(BF16)
                else:
                    gin_ref[rows_of(h), at] = result.astype(BF16)
                return carry

            lax.fori_loop(0, height, final_step, 0)

    def relay():
        @pl.when((core == 0) & has_above)
        def _():
            to_below.wait_recv()
            pass_above.start()

        @pl.when((core == 1) & has_below)
        def _():
            to_above.wait_recv()
            pass_below.start()

    def edges():
        @pl.when((core == 1) & has_above)
        def _():
            pass_above.wait_recv()

        @pl.when((core == 0) & has_below)
        def _():
            pass_below.wait_recv()

        transpose(0)
        transpose(tall + 1)

    def shifts():
        lax.fori_loop(0, tall, shift, 0)

    named = {"shift": shifts, "relay": relay, "edges": edges, "grad": gradients, "fin1": finish,
        "fin0": functools.partial(half_finish, 0),
    }

    def perform(name):
        if name in named:
            return named[name]()
        if name.startswith("conv"):
            j = int(name[4:])
            return conv(j) if j < height else None
        t, k = int(name[1]), int(name[2])
        if name[0] == "b":
            stage_b(t, k)
        elif name[0] == "c":
            for j in range(2, bits - 1):
                stage_m(t, k, j)
            stage_c(t, k)
        else:
            stage_d(t, k)

    def run(t, carry):
        multiply(t)
        for k in range(mine):
            stage_a(t, k)
        for step, names in enumerate(PLAN):
            if names:
                @pl.when(t == step)
                def _():
                    for name in names:
                        perform(name)
        return carry

    lax.fori_loop(0, TAPS, run, 0)
    for name in REST:
        perform(name)

    push_gin.wait_recv()

    def collect(h, carry):
        gin_ref[rows_of(h), pl.ds(mate_cols, half)] = gin_r[rows_of(h), :]
        return carry

    lax.fori_loop(0, height, collect, 0)

    for j, (source, target) in enumerate(((sa, ra), (sb, rb), (sm, rm), (sc, rc), (hs, hr))):
        if j != 2 or bits > 3:
            remote(source, target, out_send.at[j], out_send.at[j], mate).wait_send()
    push_feat.wait_send()
    push_gout.wait_send()
    push_gin.wait_send()
    stat_drain()
    tops_drain()
    sums_drain()

    @pl.when((core == 0) & has_above)
    def _():
        to_above.wait_send()
        pass_above.wait_send()

    @pl.when((core == 1) & has_below)
    def _():
        to_below.wait_send()
        pass_below.wait_send()


def hand_over(gin, fg, sums, gin_out, fg_out, gain_out, bias_out, sem):
    copies = (
        pltpu.make_async_copy(gin, gin_out, sem.at[0]),
        pltpu.make_async_copy(fg, fg_out, sem.at[1]),
    )
    for copy in copies:
        copy.start()
    chunks = sums.shape[0] // 2
    for c in range(chunks):
        cols = slice(c * LANES, (c + 1) * LANES)
        bias_out[:, cols] = sums[c:c + 1, :]
        gain_out[:, cols] = sums[chunks + c:chunks + c + 1, :]
    for copy in copies:
        copy.wait()


def local(n, features, grad_out, filters, norm_gain, norm_bias):
    height, width, channels = features.shape
    slab = height * width
    area, half = 2 * slab, channels // 2
    block, chips, chunks = channels // n, n // 2, channels // LANES
    mine = chunks // 2
    by_tap = filters.transpose(1, 2, 0, 3).reshape(TAPS, channels, channels)
    dma = pltpu.SemaphoreType.DMA
    hbm, vmem = pl.BlockSpec(memory_space=pltpu.HBM), pl.BlockSpec(memory_space=pltpu.VMEM)
    lots = dma((TAPS, mine))
    bits, middle = chips.bit_length() - 1, max(1, chips // 4 - 2)
    grad_in, filter_grad, sums = pl.pallas_call(
        functools.partial(kernel, n, height, width, channels),
        out_shape=(
            jax.ShapeDtypeStruct((slab, channels), BF16),
            jax.ShapeDtypeStruct((TAPS, block, channels), F32),
            jax.ShapeDtypeStruct((2 * chunks, LANES), F32),
        ),
        in_specs=[hbm] * 5,
        out_specs=(vmem, vmem, vmem),
        scratch_shapes=[
            pltpu.VMEM((slab, channels), BF16),
            pltpu.VMEM((area, half), BF16),
            pltpu.VMEM((area + 2 * width, channels), BF16),
            pltpu.VMEM((TAPS, channels, half), BF16),
            pltpu.VMEM((channels, area + 2 * width), BF16),
            pltpu.VMEM((3, area, half), BF16),
            pltpu.VMEM((area, half), F32),
            pltpu.VMEM((TAPS, chips, 2 * block, half), F32),
            pltpu.VMEM((TAPS, mine, chips // 2, 2 * block, LANES), BF16),
            pltpu.VMEM((TAPS, mine, chips // 2, 2 * block, LANES), BF16),
            pltpu.VMEM((TAPS, mine, chips // 4, 2 * block, LANES), BF16),
            pltpu.VMEM((TAPS, mine, chips // 4, 2 * block, LANES), BF16),
            pltpu.VMEM((TAPS, mine, middle, 2 * block, LANES), BF16),
            pltpu.VMEM((TAPS, mine, middle, 2 * block, LANES), BF16),
            pltpu.VMEM((TAPS, mine, 2, block, LANES), BF16),
            pltpu.VMEM((TAPS, mine, 2, block, LANES), BF16),
            pltpu.VMEM((TAPS, mine, block, LANES), F32),
            pltpu.VMEM((TAPS, mine, block, LANES), F32),
            pltpu.VMEM((2, block, LANES), F32),
            pltpu.VMEM((slab, half), BF16),
            pltpu.VMEM((slab, half), BF16),
            pltpu.VMEM((n, 1, LANES), F32),
            pltpu.VMEM((n, 1, LANES), F32),
            pltpu.VMEM((n, 2 * mine, LANES), F32),
            pltpu.VMEM((1, channels), F32),
            pltpu.VMEM((1, channels), F32),
            dma((height,)), dma((5,)), dma((3,)), dma((3,)), dma((2,)), dma((2,)),
            dma((3,)), dma((3,)),
            dma((5,)), lots, lots, dma((TAPS, mine, bits - 3) if bits > 3 else (1,)), lots,
        ],
        compiler_params=pltpu.CompilerParams(
            collective_id=0, has_side_effects=True, vmem_limit_bytes=MAIN * 1024 * 1024
        ),
        name="block_backward",
    )(
        *(
            pltpu.with_memory_space_constraint(x, pltpu.HBM)
            for x in (
                features.reshape(slab, channels), grad_out.reshape(slab, channels), by_tap,
                norm_gain.reshape(1, channels), norm_bias.reshape(1, channels),
            )
        ),
    )
    grad_in, filter_grad, gain_grad, bias_grad = pl.pallas_call(
        hand_over,
        out_shape=(
            jax.ShapeDtypeStruct((slab, channels), BF16),
            jax.ShapeDtypeStruct((TAPS, block, channels), F32),
            jax.ShapeDtypeStruct((1, channels), F32),
            jax.ShapeDtypeStruct((1, channels), F32),
        ),
        in_specs=[vmem, vmem, vmem],
        out_specs=(hbm, hbm, vmem, vmem),
        scratch_shapes=[dma((2,))],
        compiler_params=pltpu.CompilerParams(vmem_limit_bytes=8 * 1024 * 1024),
        name="hand_over",
    )(grad_in, filter_grad, sums)
    return (
        grad_in.reshape(height, width, channels),
        filter_grad.transpose(1, 0, 2).reshape(block, 3, 3, channels),
        gain_grad.reshape(channels),
        bias_grad.reshape(channels),
    )


def solution(mesh):
    slabs = P(("parts", "rows"), None, None)
    return jax.shard_map(
        functools.partial(local, mesh.shape["rows"]),
        mesh=mesh,
        in_specs=(slabs, slabs, P(), P(), P()),
        out_specs=(slabs, P(("parts", "rows"), None, None, None), P("parts"), P("parts")),
        check_vma=False,
    )
```

```python
import functools
import math

import jax
import jax.numpy as jnp
from jax import lax
from jax.experimental import pallas as pl
from jax.experimental.pallas import tpu as pltpu
from jax.sharding import PartitionSpec as P

GROUPS = 32
LANES = 128
POWER = 9
TAPS = 9
SWAPPED = 5
TURNED = 2
PLAN = (("shift", ), (), ("relay_b", "conv1", "edge_b", ), ("b00", "b01", ), ("b10", "b11", "relay_a", ), ("conv2", "b20", "edge_a", ), ("b30", "conv3", "b40", "c00", ), ("grad", "b50", "c10", "b51", ), ("b21", "b31", "b41", "c01", "c11", "b60", "c20", "c30", ))
REST = ("b61", "c40", "b70", "c50", "b71", "c51", "c60", "b80", "c61", "d00", "d10", "b81", "c70", "d20", "d30", "c21", "fin1", "c71", "c31", "c41", "fin0", "c80", "c81", "d40", "d50", "d51", "d60", "d61", "d01", "d11", "d70", "d21", "d71", "d31", "d41", "d80", "d81", )
MAIN = 40
EPSILON = 1e-06
GAIN_MAX = 1.75
BIAS_MAX = 1.0
MESH = pl.DeviceIdType.MESH
F32 = jnp.float32
BF16 = jnp.bfloat16


def encode(value):
    square = value * value
    fourth = square * square
    return (fourth * fourth * value).astype(BF16)


def decode(coded):
    wide = coded.astype(F32)
    root = jnp.exp2(jnp.log2(jnp.maximum(jnp.abs(wide), 1e-38)) * (1.0 / POWER))
    root = jnp.where(jnp.abs(wide) < 1e-37, 0.0, root)
    return jnp.where(wide < 0.0, -root, root)


def group_sum(row, per_group):
    value = jnp.broadcast_to(row, (8, LANES))
    lane = lax.broadcasted_iota(jnp.int32, (8, LANES), 1)
    step = 1
    while step < per_group:
        low = pltpu.roll(value, step, 1)
        high = pltpu.roll(value, LANES - step, 1)
        value = value + jnp.where((lane & step) != 0, low, high)
        step *= 2
    return value[0:1]


def kernel(
    n, height, width, channels,
    feat_hbm, gout_hbm, filt_hbm, gain_hbm, bias_hbm,
    gin_ref, fg_ref, sums_ref,
    feat, featc, gext, filt, gt, act, gact, part, sa, ra, sb, rb, sm, rm, sc, rc, hs, hr, both,
    gin_s, gin_r, stat, tops, sums, gain_ref, bias_ref,
    feat_sem, local_sem, push_send, push_recv, halo_send, halo_recv,
    share_send, share_recv,
    out_send, a_recv, b_recv, m_recv, c_recv,
):
    me = lax.axis_index("rows")
    core, chip = lax.rem(me, 2), lax.div(me, 2)
    mate = me + 1 - 2 * core
    chips = n // 2
    bits = chips.bit_length() - 1
    bit = [lax.rem(lax.div(chip, 1 << j), 2) for j in range(bits)]
    across = [(2 << j) * (1 - 2 * bit[j]) for j in range(bits)]
    block = channels // n
    half = channels // 2
    chunks = channels // LANES
    mine = half // LANES
    per_group = channels // GROUPS
    slab = height * width
    tall = 2 * height
    area = 2 * slab
    pixels = slab * n
    members = pixels * per_group
    own = pl.multiple_of(core * slab, slab)
    other = pl.multiple_of((1 - core) * slab, slab)
    my_cols = pl.multiple_of(core * half, LANES)
    mate_cols = pl.multiple_of((1 - core) * half, LANES)

    def remote(src, dst, send, recv, target):
        return pltpu.make_async_remote_copy(
            src_ref=src, dst_ref=dst, send_sem=send, recv_sem=recv,
            device_id={"rows": target}, device_id_type=MESH,
        )

    def peer(k):
        return lax.rem(me + k, n)

    def rows_of(h):
        return pl.ds(pl.multiple_of(h * width, width), width)

    in_feat = [
        pltpu.make_async_copy(
            feat_hbm.at[pl.ds(h * width, width)], feat.at[pl.ds(h * width, width)], feat_sem.at[h]
        )
        for h in range(height)
    ]
    in_gout = pltpu.make_async_copy(
        gout_hbm, gext.at[pl.ds(width + own, slab)], local_sem.at[0]
    )
    in_half = pltpu.make_async_copy(
        feat_hbm.at[:, pl.ds(my_cols, half)], featc.at[pl.ds(own, slab)], local_sem.at[1]
    )
    in_filt = pltpu.make_async_copy(
        filt_hbm.at[:, :, pl.ds(my_cols, half)], filt, local_sem.at[2]
    )
    in_gain = pltpu.make_async_copy(gain_hbm, gain_ref, local_sem.at[3])
    in_bias = pltpu.make_async_copy(bias_hbm, bias_ref, local_sem.at[4])
    for copy in in_feat:
        copy.start()

    barrier = pltpu.get_barrier_semaphore()

    def greet(k, carry):
        pl.semaphore_signal(barrier, inc=1, device_id={"rows": peer(k)}, device_id_type=MESH)
        return carry

    lax.fori_loop(1, n, greet, 0)

    in_gout.start()

    def shared(buffer, j):
        def copy(k):
            return remote(
                buffer.at[me], buffer.at[me], share_send.at[j], share_recv.at[j], peer(k)
            )

        def start():
            def body(k, carry):
                copy(k).start()
                return carry
            lax.fori_loop(1, n, body, 0)

        others = buffer.at[pl.ds(0, n - 1)]
        every = remote(others, others, share_send.at[j], share_recv.at[j], mate)
        return start, every.wait_recv, every.wait_send

    stat_start, stat_wait, stat_drain = shared(stat, 0)
    tops_start, tops_wait, tops_drain = shared(tops, 1)
    sums_start, sums_wait, sums_drain = shared(sums, 2)

    lane = lax.broadcasted_iota(jnp.int32, (1, LANES), 1)
    slot = lane & (per_group - 1)
    totals = [jnp.zeros((8, LANES), F32) for _ in range(chunks)]
    squares = [jnp.zeros((8, LANES), F32) for _ in range(chunks)]
    for h in range(height):
        in_feat[h].wait()
        for c in range(chunks):
            x = feat[h * width:(h + 1) * width, c * LANES:(c + 1) * LANES].astype(F32)
            x = x.reshape(width // 8, 8, LANES)
            totals[c] = totals[c] + x.sum(0)
            squares[c] = squares[c] + (x * x).sum(0)
    in_half.start()
    in_filt.start()
    in_gain.start()
    in_bias.start()
    packed = jnp.zeros((1, LANES), F32)
    for c in range(chunks):
        total = group_sum(totals[c].sum(0, keepdims=True), per_group)
        square = group_sum(squares[c].sum(0, keepdims=True), per_group)
        packed = packed + jnp.where(slot == c, total, 0.0)
        packed = packed + jnp.where(slot == chunks + c, square, 0.0)
    stat[me] = packed

    in_gout.wait()

    def top_step(h, carry):
        g = jnp.abs(gext[rows_of(1 + core * height + h), :])
        return jnp.maximum(carry, g.reshape(width // 16, 16, channels).max(0))

    largest = lax.fori_loop(0, height, top_step, jnp.zeros((16, channels), BF16))
    largest = largest.astype(F32).max(0, keepdims=True)
    top = jnp.zeros((1, LANES), F32)
    for c in range(chunks):
        top = jnp.maximum(top, largest[:, c * LANES:(c + 1) * LANES])
    tops[me] = top
    push_feat = remote(
        feat.at[:, pl.ds(mate_cols, half)], featc.at[pl.ds(own, slab)],
        push_send.at[0], push_recv.at[0], mate,
    )
    push_gout = remote(
        gext.at[pl.ds(width + own, slab)], gext.at[pl.ds(width + own, slab)],
        push_send.at[1], push_recv.at[1], mate,
    )
    pl.semaphore_wait(barrier, n - 1)
    stat_start()
    tops_start()
    push_gout.start()
    push_feat.start()

    above, below = pl.ds(0, width), pl.ds((tall + 1) * width, width)
    first, last = pl.ds(width, width), pl.ds(tall * width, width)

    to_above = remote(gext.at[first], gext.at[below], halo_send.at[0], halo_recv.at[0], me - 1)
    to_below = remote(gext.at[last], gext.at[above], halo_send.at[0], halo_recv.at[0], me + 1)
    pass_above = remote(gext.at[above], gext.at[above], halo_send.at[1], halo_recv.at[1], mate)
    pass_below = remote(gext.at[below], gext.at[below], halo_send.at[1], halo_recv.at[1], mate)
    has_above, has_below = chip > 0, chip < chips - 1

    @pl.when(chip == 0)
    def _():
        gext[above, :] = jnp.zeros((width, channels), BF16)

    @pl.when(chip == chips - 1)
    def _():
        gext[below, :] = jnp.zeros((width, channels), BF16)


    @pl.when((core == 0) & has_above)
    def _():
        to_above.start()

    @pl.when((core == 1) & has_below)
    def _():
        to_below.start()


    column = lax.broadcasted_iota(jnp.int32, (width, LANES), 0)

    def from_left(x):
        return jnp.where(column > 0, pltpu.roll(x, 1, 0), 0.0)

    def from_right(x):
        return jnp.where(column < width - 1, pltpu.roll(x, width - 1, 0), 0.0)

    def conv(j):
        turned = core * (height - 2 - 2 * j) + j
        inner = lax.div(height - 1 - j + tall - 3, tall - 2)
        first_row = 1 + 2 * (inner * turned + (1 - inner) * j)
        where = [first_row, lax.rem(first_row + 1, tall)]
        ys = [[], []]
        for s in range(3):
            for m in range(2):
                y = None
                for r in range(3):
                    d = jnp.dot(
                        gext[rows_of(where[m] - r + 2), :], filt[3 * r + s],
                        preferred_element_type=F32,
                    )
                    y = d if y is None else y + d
                ys[m].append(y)
        for m in range(2):
            for k in range(mine):
                sub = slice(k * LANES, (k + 1) * LANES)
                y = ys[m]
                gact[rows_of(where[m]), sub] = (
                    y[1][:, sub] + from_right(y[0][:, sub]) + from_left(y[2][:, sub])
                )

    def transpose(e):
        start = pl.multiple_of(e * width, width)
        gt[:, pl.ds(start, width)] = gext[pl.ds(start, width), :].T

    def transposes(base, count):
        def body(e, carry):
            transpose(base + e)
            return carry
        lax.fori_loop(0, count, body, 0)

    transposes(1 + core * height, height)
    in_filt.wait()
    conv(0)

    push_gout_in = remote(
        gext.at[pl.ds(width + other, slab)], gext.at[pl.ds(width + other, slab)],
        push_send.at[1], push_recv.at[1], mate,
    )
    push_feat_in = remote(
        feat.at[:, pl.ds(mate_cols, half)], featc.at[pl.ds(other, slab)],
        push_send.at[0], push_recv.at[0], mate,
    )
    push_gout_in.wait_recv()
    transposes(1 + (1 - core) * height, height)

    in_half.wait()
    in_gain.wait()
    in_bias.wait()
    push_feat_in.wait_recv()

    stat_wait()
    total_stat = stat[...].sum(0)
    means, invs, gains, biases = [], [], [], []
    for k in range(mine):
        which = core * mine + k
        total = group_sum(jnp.where(slot == which, total_stat, 0.0), per_group)
        square = group_sum(jnp.where(slot == chunks + which, total_stat, 0.0), per_group)
        mean = total / members
        means.append(mean)
        invs.append(lax.rsqrt(square / members - mean * mean + EPSILON))
        at = pl.ds(pl.multiple_of(my_cols + k * LANES, LANES), LANES)
        gains.append(gain_ref[:, at])
        biases.append(bias_ref[:, at])

    def forward(rows, k):
        cols = slice(k * LANES, (k + 1) * LANES)
        normalized = (featc[rows, cols].astype(F32) - means[k]) * invs[k]
        normed = normalized * gains[k] + biases[k]
        return normalized, normed, 1.0 / (1.0 + jnp.exp(-normed))

    def activate(h, carry):
        rows = rows_of(h)
        for k in range(mine):
            _, normed, sig = forward(rows, k)
            act[1, rows, k * LANES:(k + 1) * LANES] = (normed * sig).astype(BF16)
        return carry

    lax.fori_loop(0, tall, activate, 0)

    tops_wait()
    gmax = jnp.max(tops[...].max(0), axis=1, keepdims=True)
    bound = GAIN_MAX * math.sqrt(float(pixels) * float(members)) + BIAS_MAX * pixels
    reach = bound * jnp.maximum(gmax, 1e-30) * (2.0 ** -13.9)
    scale = 1.0 / reach

    def shift(h, carry):
        rows = rows_of(h)
        for k in range(mine):
            cols = slice(k * LANES, (k + 1) * LANES)
            a = act[1, rows, cols].astype(F32)
            act[0, rows, cols] = from_left(a).astype(BF16)
            act[2, rows, cols] = from_right(a).astype(BF16)
        return carry

    def multiply(t):
        s = lax.rem(1 + 2 * lax.rem(t, 3), 3)
        r = lax.rem(1 + 2 * lax.div(t, 3), 3)
        start = pl.multiple_of((2 - r) * width, LANES)
        for m in range(2):
            result = jnp.dot(
                gt[m * half:(m + 1) * half, pl.ds(start, area)], act[s],
                preferred_element_type=F32,
            )
            part[t, m * (chips // 2):(m + 1) * (chips // 2)] = result.reshape(
                chips // 2, 2 * block, half
            )

    def reached(t, least):
        return lax.div(t + TAPS - least, TAPS)

    def swapped(t, k):
        return k * (1 - reached(t, SWAPPED))

    def order_of(t, k):
        if k == 0 or t >= SWAPPED:
            return list(range(bits))
        return [1, 2, 0] + list(range(3, bits)) if t < TURNED else [1, 0] + list(range(2, bits))

    def copy_a(t, k):
        kind = swapped(t, k)
        target = me + kind * across[1] + (1 - kind) * across[0]
        return remote(sa.at[t, k], ra.at[t, k], out_send.at[0], a_recv.at[t, k], target)

    def copy_b(t, k):
        target = me + across[order_of(t, k)[1]]
        return remote(sb.at[t, k], rb.at[t, k], out_send.at[1], b_recv.at[t, k], target)

    def copy_m(t, k, j):
        at = pl.ds(chips // 4 - (chips >> j), chips >> (j + 1))
        return remote(
            sm.at[t, k, at], rm.at[t, k, at],
            out_send.at[2], m_recv.at[t, k, j - 2], me + across[order_of(t, k)[j]],
        )

    def copy_c(t, k, way, source):
        target = lax.div(me + across[order_of(t, k)[-1]], 2) * 2 + way
        return remote(
            sc.at[t, k, way], rc.at[t, k, source],
            out_send.at[3], c_recv.at[t, k], target,
        )

    def copy_h(t, k):
        return remote(hs.at[t, k], hr.at[t, k], out_send.at[4], c_recv.at[t, k], mate)

    def lanes_of(k):
        return slice(k * LANES, (k + 1) * LANES)

    def stage_a(t, k):
        kind = swapped(t, k)
        for w in range(chips // 2):
            u, v = w >> 1, w & 1
            dest = u * 4 + kind * (2 * (1 - bit[1]) + v) + (1 - kind) * (2 * v + 1 - bit[0])
            sa[t, k, w] = encode(part[t, dest, :, lanes_of(k)] * scale)
        copy_a(t, k).start()

    def hop(t, k, i):
        order = order_of(t, k)
        before = sorted(set(range(bits)) - set(order[:i]))
        rest = [b for b in before if b != order[i]]
        here = bit[order[i]]
        if i == 1:
            copy_a(t, k).wait_recv()
            buffer, base = ra, 0
        elif i == 2:
            copy_b(t, k).wait_recv()
            buffer, base = rb, 0
        else:
            copy_m(t, k, i - 1).wait_recv()
            buffer, base = rm, chips // 4 - (chips >> (i - 1))

        def place(w, side):
            spot = side * (1 << order[i])
            for b in order[:i]:
                spot = spot + bit[b] * (1 << b)
            return spot + sum(((w >> j) & 1) << b for j, b in enumerate(rest))

        def value(w, side, rows):
            index = base + side * (1 << before.index(order[i]))
            index = index + sum(((w >> j) & 1) << before.index(b) for j, b in enumerate(rest))
            kept = part[t, place(w, side), rows, lanes_of(k)]
            kept = kept * scale if i == 1 else kept
            return kept + decode(buffer[t, k, index, rows])

        if i < bits - 1:
            out = sb if i == 1 else sm
            first_slot = 0 if i == 1 else chips // 4 - (chips >> i)
            for w in range(chips >> (i + 1)):
                out[t, k, first_slot + w] = encode(value(w, 1 - here, slice(None)))
            (copy_b(t, k) if i == 1 else copy_m(t, k, i)).start()
            for w in range(chips >> (i + 1)):
                part[t, place(w, here), :, lanes_of(k)] = value(w, here, slice(None))
            return
        for way in range(2):
            rows = slice(way * block, (way + 1) * block)
            sc[t, k, way] = encode(value(0, 1 - here, rows))
            copy_c(t, k, way, core).start()
        hs[t, k] = value(0, here, pl.ds(pl.multiple_of((1 - core) * block, block), block))
        copy_h(t, k).start()
        rows = pl.ds(pl.multiple_of(core * block, block), block)
        part[t, chip, rows, lanes_of(k)] = value(0, here, rows)

    def stage_d(t, k):
        tap = 3 * lax.rem(1 + 2 * lax.div(t, 3), 3) + lax.rem(1 + 2 * lax.rem(t, 3), 3)
        rows = pl.ds(pl.multiple_of(core * block, block), block)
        remote(both, both, out_send.at[3], c_recv.at[t, k], mate).wait_recv()
        total = part[t, chip, rows, lanes_of(k)]
        total = total + decode(rc[t, k, core])
        at = pl.ds(pl.multiple_of(my_cols + k * LANES, LANES), LANES)
        fg_ref[tap, :, at] = total * (reach / pixels)
        total = hr[t, k] + decode(rc[t, k, 1 - core])
        at = pl.ds(pl.multiple_of(mate_cols + k * LANES, LANES), LANES)
        fg_ref[tap, :, at] = total * (reach / pixels)

    def gradients():
        for k in range(mine):
            cols = lanes_of(k)

            def grad_step(h, carry):
                bias_sum, gain_sum = carry
                rows = rows_of(h)
                normalized, normed, sig = forward(rows, k)
                pre = gact[rows, cols] * (sig * (1.0 + normed * (1.0 - sig)))
                gact[rows, cols] = pre
                return (
                    bias_sum + pre.reshape(width // 8, 8, LANES).sum(0),
                    gain_sum + (pre * normalized).reshape(width // 8, 8, LANES).sum(0),
                )

            zero = jnp.zeros((8, LANES), F32)
            bias_sum, gain_sum = lax.fori_loop(0, tall, grad_step, (zero, zero))
            sums[me, k:k + 1, :] = bias_sum.sum(0, keepdims=True)
            sums[me, mine + k:mine + k + 1, :] = gain_sum.sum(0, keepdims=True)
        sums_start()

    push_gin = remote(gin_s, gin_r, push_send.at[2], push_recv.at[2], mate)

    def finish():
        sums_wait()
        everyone = sums[...].reshape(chips, 2, 2 * mine, LANES).sum(0)
        for c in range(2):
            for k in range(mine):
                sums_ref[c * mine + k:c * mine + k + 1, :] = everyone[c, k:k + 1]
                sums_ref[chunks + c * mine + k:chunks + c * mine + k + 1, :] = (
                    everyone[c, mine + k:mine + k + 1]
                )
        half_finish(1)
        push_gin.start()

    def half_finish(side):
        base = (1 - core if side else core) * height
        for k in range(mine):
            mean_grad = group_sum(
                gains[k] * sums_ref[pl.ds(core * mine + k, 1), :], per_group
            ) / members
            mean_cross = group_sum(
                gains[k] * sums_ref[pl.ds(chunks + core * mine + k, 1), :], per_group
            ) / members
            at = pl.ds(pl.multiple_of(my_cols + k * LANES, LANES), LANES)

            def final_step(h, carry):
                rows = rows_of(base + h)
                cols = lanes_of(k)
                normalized = (featc[rows, cols].astype(F32) - means[k]) * invs[k]
                result = invs[k] * (gact[rows, cols] * gains[k] - mean_grad - normalized * mean_cross)
                if side:
                    gin_s[rows_of(h), cols] = result.astype(BF16)
                else:
                    gin_ref[rows_of(h), at] = result.astype(BF16)
                return carry

            lax.fori_loop(0, height, final_step, 0)

    def relay_below():
        @pl.when((core == 1) & has_below)
        def _():
            to_above.wait_recv()
            pass_below.start()

    def relay_above():
        @pl.when((core == 0) & has_above)
        def _():
            to_below.wait_recv()
            pass_above.start()

    def edge_below():
        @pl.when((core == 0) & has_below)
        def _():
            pass_below.wait_recv()

        transpose(tall + 1)

    def edge_above():
        @pl.when((core == 1) & has_above)
        def _():
            pass_above.wait_recv()

        transpose(0)

    def shifts():
        lax.fori_loop(0, tall, shift, 0)

    named = {"shift": shifts, "relay_b": relay_below, "relay_a": relay_above,
        "edge_b": edge_below, "edge_a": edge_above, "grad": gradients, "fin1": finish,
        "fin0": functools.partial(half_finish, 0),
    }

    def perform(name):
        if name in named:
            return named[name]()
        if name.startswith("conv"):
            j = int(name[4:])
            return conv(j) if j < height else None
        t, k = int(name[1]), int(name[2])
        if name[0] == "b":
            hop(t, k, 1)
        elif name[0] == "c":
            for i in range(2, bits):
                hop(t, k, i)
        else:
            stage_d(t, k)

    def run(t, carry):
        multiply(t)
        for k in range(mine):
            stage_a(t, k)
        for step, names in enumerate(PLAN):
            if names:
                @pl.when(t == step)
                def _():
                    for name in names:
                        perform(name)
        return carry

    lax.fori_loop(0, TAPS, run, 0)
    for name in REST:
        perform(name)

    push_gin.wait_recv()

    def collect(h, carry):
        gin_ref[rows_of(h), pl.ds(mate_cols, half)] = gin_r[rows_of(h), :]
        return carry

    lax.fori_loop(0, height, collect, 0)

    for j, (source, target) in enumerate(((sa, ra), (sb, rb), (sm, rm), (sc, rc), (hs, hr))):
        if j != 2 or bits > 3:
            remote(source, target, out_send.at[j], out_send.at[j], mate).wait_send()
    push_feat.wait_send()
    push_gout.wait_send()
    push_gin.wait_send()
    stat_drain()
    tops_drain()
    sums_drain()

    @pl.when((core == 0) & has_above)
    def _():
        to_above.wait_send()
        pass_above.wait_send()

    @pl.when((core == 1) & has_below)
    def _():
        to_below.wait_send()
        pass_below.wait_send()


def hand_over(gin, fg, sums, gin_out, fg_out, gain_out, bias_out, sem):
    copies = (
        pltpu.make_async_copy(gin, gin_out, sem.at[0]),
        pltpu.make_async_copy(fg, fg_out, sem.at[1]),
    )
    for copy in copies:
        copy.start()
    chunks = sums.shape[0] // 2
    for c in range(chunks):
        cols = slice(c * LANES, (c + 1) * LANES)
        bias_out[:, cols] = sums[c:c + 1, :]
        gain_out[:, cols] = sums[chunks + c:chunks + c + 1, :]
    for copy in copies:
        copy.wait()


def local(n, features, grad_out, filters, norm_gain, norm_bias):
    height, width, channels = features.shape
    slab = height * width
    area, half = 2 * slab, channels // 2
    block, chips, chunks = channels // n, n // 2, channels // LANES
    mine = chunks // 2
    by_tap = filters.transpose(1, 2, 0, 3).reshape(TAPS, channels, channels)
    dma = pltpu.SemaphoreType.DMA
    hbm, vmem = pl.BlockSpec(memory_space=pltpu.HBM), pl.BlockSpec(memory_space=pltpu.VMEM)
    lots = dma((TAPS, mine))
    bits, middle = chips.bit_length() - 1, max(1, chips // 4 - 2)
    grad_in, filter_grad, sums = pl.pallas_call(
        functools.partial(kernel, n, height, width, channels),
        out_shape=(
            jax.ShapeDtypeStruct((slab, channels), BF16),
            jax.ShapeDtypeStruct((TAPS, block, channels), F32),
            jax.ShapeDtypeStruct((2 * chunks, LANES), F32),
        ),
        in_specs=[hbm] * 5,
        out_specs=(vmem, vmem, vmem),
        scratch_shapes=[
            pltpu.VMEM((slab, channels), BF16),
            pltpu.VMEM((area, half), BF16),
            pltpu.VMEM((area + 2 * width, channels), BF16),
            pltpu.VMEM((TAPS, channels, half), BF16),
            pltpu.VMEM((channels, area + 2 * width), BF16),
            pltpu.VMEM((3, area, half), BF16),
            pltpu.VMEM((area, half), F32),
            pltpu.VMEM((TAPS, chips, 2 * block, half), F32),
            pltpu.VMEM((TAPS, mine, chips // 2, 2 * block, LANES), BF16),
            pltpu.VMEM((TAPS, mine, chips // 2, 2 * block, LANES), BF16),
            pltpu.VMEM((TAPS, mine, chips // 4, 2 * block, LANES), BF16),
            pltpu.VMEM((TAPS, mine, chips // 4, 2 * block, LANES), BF16),
            pltpu.VMEM((TAPS, mine, middle, 2 * block, LANES), BF16),
            pltpu.VMEM((TAPS, mine, middle, 2 * block, LANES), BF16),
            pltpu.VMEM((TAPS, mine, 2, block, LANES), BF16),
            pltpu.VMEM((TAPS, mine, 2, block, LANES), BF16),
            pltpu.VMEM((TAPS, mine, block, LANES), F32),
            pltpu.VMEM((TAPS, mine, block, LANES), F32),
            pltpu.VMEM((2, block, LANES), F32),
            pltpu.VMEM((slab, half), BF16),
            pltpu.VMEM((slab, half), BF16),
            pltpu.VMEM((n, 1, LANES), F32),
            pltpu.VMEM((n, 1, LANES), F32),
            pltpu.VMEM((n, 2 * mine, LANES), F32),
            pltpu.VMEM((1, channels), F32),
            pltpu.VMEM((1, channels), F32),
            dma((height,)), dma((5,)), dma((3,)), dma((3,)), dma((2,)), dma((2,)),
            dma((3,)), dma((3,)),
            dma((5,)), lots, lots, dma((TAPS, mine, bits - 3) if bits > 3 else (1,)), lots,
        ],
        compiler_params=pltpu.CompilerParams(
            collective_id=0, has_side_effects=True, vmem_limit_bytes=MAIN * 1024 * 1024
        ),
        name="block_backward",
    )(
        *(
            pltpu.with_memory_space_constraint(x, pltpu.HBM)
            for x in (
                features.reshape(slab, channels), grad_out.reshape(slab, channels), by_tap,
                norm_gain.reshape(1, channels), norm_bias.reshape(1, channels),
            )
        ),
    )
    grad_in, filter_grad, gain_grad, bias_grad = pl.pallas_call(
        hand_over,
        out_shape=(
            jax.ShapeDtypeStruct((slab, channels), BF16),
            jax.ShapeDtypeStruct((TAPS, block, channels), F32),
            jax.ShapeDtypeStruct((1, channels), F32),
            jax.ShapeDtypeStruct((1, channels), F32),
        ),
        in_specs=[vmem, vmem, vmem],
        out_specs=(hbm, hbm, vmem, vmem),
        scratch_shapes=[dma((2,))],
        compiler_params=pltpu.CompilerParams(vmem_limit_bytes=8 * 1024 * 1024),
        name="hand_over",
    )(grad_in, filter_grad, sums)
    return (
        grad_in.reshape(height, width, channels),
        filter_grad.transpose(1, 0, 2).reshape(block, 3, 3, channels),
        gain_grad.reshape(channels),
        bias_grad.reshape(channels),
    )


def solution(mesh):
    slabs = P(("parts", "rows"), None, None)
    return jax.shard_map(
        functools.partial(local, mesh.shape["rows"]),
        mesh=mesh,
        in_specs=(slabs, slabs, P(), P(), P()),
        out_specs=(slabs, P(("parts", "rows"), None, None, None), P("parts"), P("parts")),
        check_vma=False,
    )
```

```python
import functools
import math

import jax
import jax.numpy as jnp
from jax import lax
from jax.experimental import pallas as pl
from jax.experimental.pallas import tpu as pltpu
from jax.sharding import PartitionSpec as P

GROUPS = 32
LANES = 128
POWER = 9
TAPS = 9
SWAPPED = 5
TURNED = 2
PLAN = (("shift", ), (), ("relay_b", "conv1", "edge_b", ), ("b00", "b01", ), ("b10", "b11", "relay_a", ), ("conv2", "b20", "edge_a", ), ("b30", "conv3", "b40", "c00", ), ("grad", "b50", "c10", "b51", ), ("b21", "b31", "b41", "c01", "c11", "b60", "c20", "c30", ))
REST = ("b61", "c40", "b70", "c50", "b71", "c51", "c60", "b80", "c61", "d00", "d10", "b81", "c70", "d20", "d30", "c21", "fin1", "c71", "c31", "c41", "fin0", "c80", "c81", "d40", "d50", "d51", "d60", "d61", "d01", "d11", "d70", "d21", "d71", "d31", "d41", "d80", "d81", )
MAIN = 40
EPSILON = 1e-06
GAIN_MAX = 1.75
BIAS_MAX = 1.0
MESH = pl.DeviceIdType.MESH
F32 = jnp.float32
BF16 = jnp.bfloat16


def encode(value):
    square = value * value
    fourth = square * square
    return (fourth * fourth * value).astype(BF16)


def decode(coded):
    wide = coded.astype(F32)
    root = jnp.exp2(jnp.log2(jnp.maximum(jnp.abs(wide), 1e-38)) * (1.0 / POWER))
    root = jnp.where(jnp.abs(wide) < 1e-37, 0.0, root)
    return jnp.where(wide < 0.0, -root, root)


def group_sum(row, per_group):
    value = jnp.broadcast_to(row, (8, LANES))
    lane = lax.broadcasted_iota(jnp.int32, (8, LANES), 1)
    step = 1
    while step < per_group:
        low = pltpu.roll(value, step, 1)
        high = pltpu.roll(value, LANES - step, 1)
        value = value + jnp.where((lane & step) != 0, low, high)
        step *= 2
    return value[0:1]


def kernel(
    n, height, width, channels,
    feat_hbm, gout_hbm, filt_hbm, gain_hbm, bias_hbm,
    gin_ref, fg_ref, gain_row, bias_row,
    feat, featc, gext, filt, gt, act, gact, part, sa, ra, sb, rb, sm, rm, sc, rc, hs, hr, both,
    gin_s, gin_r, stat, tops, sums, sums_ref, gain_ref, bias_ref,
    feat_sem, local_sem, push_send, push_recv, halo_send, halo_recv,
    share_send, share_recv,
    out_send, a_recv, b_recv, m_recv, c_recv,
):
    me = lax.axis_index("rows")
    core, chip = lax.rem(me, 2), lax.div(me, 2)
    mate = me + 1 - 2 * core
    chips = n // 2
    bits = chips.bit_length() - 1
    bit = [lax.rem(lax.div(chip, 1 << j), 2) for j in range(bits)]
    across = [(2 << j) * (1 - 2 * bit[j]) for j in range(bits)]
    block = channels // n
    half = channels // 2
    chunks = channels // LANES
    mine = half // LANES
    per_group = channels // GROUPS
    slab = height * width
    tall = 2 * height
    area = 2 * slab
    pixels = slab * n
    members = pixels * per_group
    own = pl.multiple_of(core * slab, slab)
    other = pl.multiple_of((1 - core) * slab, slab)
    my_cols = pl.multiple_of(core * half, LANES)
    mate_cols = pl.multiple_of((1 - core) * half, LANES)

    def remote(src, dst, send, recv, target):
        return pltpu.make_async_remote_copy(
            src_ref=src, dst_ref=dst, send_sem=send, recv_sem=recv,
            device_id={"rows": target}, device_id_type=MESH,
        )

    def peer(k):
        return lax.rem(me + k, n)

    def rows_of(h):
        return pl.ds(pl.multiple_of(h * width, width), width)

    in_feat = [
        pltpu.make_async_copy(
            feat_hbm.at[pl.ds(h * width, width)], feat.at[pl.ds(h * width, width)], feat_sem.at[h]
        )
        for h in range(height)
    ]
    in_gout = pltpu.make_async_copy(
        gout_hbm, gext.at[pl.ds(width + own, slab)], local_sem.at[0]
    )
    in_half = pltpu.make_async_copy(
        feat_hbm.at[:, pl.ds(my_cols, half)], featc.at[pl.ds(own, slab)], local_sem.at[1]
    )
    in_filt = pltpu.make_async_copy(
        filt_hbm.at[:, :, pl.ds(my_cols, half)], filt, local_sem.at[2]
    )
    in_gain = pltpu.make_async_copy(gain_hbm, gain_ref, local_sem.at[3])
    in_bias = pltpu.make_async_copy(bias_hbm, bias_ref, local_sem.at[4])
    for copy in in_feat:
        copy.start()

    barrier = pltpu.get_barrier_semaphore()

    def greet(k, carry):
        pl.semaphore_signal(barrier, inc=1, device_id={"rows": peer(k)}, device_id_type=MESH)
        return carry

    lax.fori_loop(1, n, greet, 0)

    in_gout.start()

    def shared(buffer, j):
        def copy(k):
            return remote(
                buffer.at[me], buffer.at[me], share_send.at[j], share_recv.at[j], peer(k)
            )

        def start():
            def body(k, carry):
                copy(k).start()
                return carry
            lax.fori_loop(1, n, body, 0)

        others = buffer.at[pl.ds(0, n - 1)]
        every = remote(others, others, share_send.at[j], share_recv.at[j], mate)
        return start, every.wait_recv, every.wait_send

    stat_start, stat_wait, stat_drain = shared(stat, 0)
    tops_start, tops_wait, tops_drain = shared(tops, 1)
    sums_start, sums_wait, sums_drain = shared(sums, 2)

    lane = lax.broadcasted_iota(jnp.int32, (1, LANES), 1)
    slot = lane & (per_group - 1)
    totals = [jnp.zeros((8, LANES), F32) for _ in range(chunks)]
    squares = [jnp.zeros((8, LANES), F32) for _ in range(chunks)]
    for h in range(height):
        in_feat[h].wait()
        for c in range(chunks):
            x = feat[h * width:(h + 1) * width, c * LANES:(c + 1) * LANES].astype(F32)
            x = x.reshape(width // 8, 8, LANES)
            totals[c] = totals[c] + x.sum(0)
            squares[c] = squares[c] + (x * x).sum(0)
    in_half.start()
    in_filt.start()
    in_gain.start()
    in_bias.start()
    packed = jnp.zeros((1, LANES), F32)
    for c in range(chunks):
        total = group_sum(totals[c].sum(0, keepdims=True), per_group)
        square = group_sum(squares[c].sum(0, keepdims=True), per_group)
        packed = packed + jnp.where(slot == c, total, 0.0)
        packed = packed + jnp.where(slot == chunks + c, square, 0.0)
    stat[me] = packed

    in_gout.wait()

    def top_step(h, carry):
        g = jnp.abs(gext[rows_of(1 + core * height + h), :])
        return jnp.maximum(carry, g.reshape(width // 16, 16, channels).max(0))

    largest = lax.fori_loop(0, height, top_step, jnp.zeros((16, channels), BF16))
    largest = largest.astype(F32).max(0, keepdims=True)
    top = jnp.zeros((1, LANES), F32)
    for c in range(chunks):
        top = jnp.maximum(top, largest[:, c * LANES:(c + 1) * LANES])
    tops[me] = top
    push_feat = remote(
        feat.at[:, pl.ds(mate_cols, half)], featc.at[pl.ds(own, slab)],
        push_send.at[0], push_recv.at[0], mate,
    )
    push_gout = remote(
        gext.at[pl.ds(width + own, slab)], gext.at[pl.ds(width + own, slab)],
        push_send.at[1], push_recv.at[1], mate,
    )
    pl.semaphore_wait(barrier, n - 1)
    stat_start()
    tops_start()
    push_gout.start()
    push_feat.start()

    above, below = pl.ds(0, width), pl.ds((tall + 1) * width, width)
    first, last = pl.ds(width, width), pl.ds(tall * width, width)

    to_above = remote(gext.at[first], gext.at[below], halo_send.at[0], halo_recv.at[0], me - 1)
    to_below = remote(gext.at[last], gext.at[above], halo_send.at[0], halo_recv.at[0], me + 1)
    pass_above = remote(gext.at[above], gext.at[above], halo_send.at[1], halo_recv.at[1], mate)
    pass_below = remote(gext.at[below], gext.at[below], halo_send.at[1], halo_recv.at[1], mate)
    has_above, has_below = chip > 0, chip < chips - 1

    @pl.when(chip == 0)
    def _():
        gext[above, :] = jnp.zeros((width, channels), BF16)

    @pl.when(chip == chips - 1)
    def _():
        gext[below, :] = jnp.zeros((width, channels), BF16)


    @pl.when((core == 0) & has_above)
    def _():
        to_above.start()

    @pl.when((core == 1) & has_below)
    def _():
        to_below.start()


    column = lax.broadcasted_iota(jnp.int32, (width, LANES), 0)

    def from_left(x):
        return jnp.where(column > 0, pltpu.roll(x, 1, 0), 0.0)

    def from_right(x):
        return jnp.where(column < width - 1, pltpu.roll(x, width - 1, 0), 0.0)

    def conv(j):
        turned = core * (height - 2 - 2 * j) + j
        inner = lax.div(height - 1 - j + tall - 3, tall - 2)
        first_row = 1 + 2 * (inner * turned + (1 - inner) * j)
        where = [first_row, lax.rem(first_row + 1, tall)]
        ys = [[], []]
        for s in range(3):
            for m in range(2):
                y = None
                for r in range(3):
                    d = jnp.dot(
                        gext[rows_of(where[m] - r + 2), :], filt[3 * r + s],
                        preferred_element_type=F32,
                    )
                    y = d if y is None else y + d
                ys[m].append(y)
        for m in range(2):
            for k in range(mine):
                sub = slice(k * LANES, (k + 1) * LANES)
                y = ys[m]
                gact[rows_of(where[m]), sub] = (
                    y[1][:, sub] + from_right(y[0][:, sub]) + from_left(y[2][:, sub])
                )

    def transpose(e):
        start = pl.multiple_of(e * width, width)
        gt[:, pl.ds(start, width)] = gext[pl.ds(start, width), :].T

    def transposes(base, count):
        def body(e, carry):
            transpose(base + e)
            return carry
        lax.fori_loop(0, count, body, 0)

    transposes(1 + core * height, height)
    in_filt.wait()
    conv(0)

    push_gout_in = remote(
        gext.at[pl.ds(width + other, slab)], gext.at[pl.ds(width + other, slab)],
        push_send.at[1], push_recv.at[1], mate,
    )
    push_feat_in = remote(
        feat.at[:, pl.ds(mate_cols, half)], featc.at[pl.ds(other, slab)],
        push_send.at[0], push_recv.at[0], mate,
    )
    push_gout_in.wait_recv()
    transposes(1 + (1 - core) * height, height)

    in_half.wait()
    in_gain.wait()
    in_bias.wait()
    push_feat_in.wait_recv()

    stat_wait()
    total_stat = stat[...].sum(0)
    means, invs, gains, biases = [], [], [], []
    for k in range(mine):
        which = core * mine + k
        total = group_sum(jnp.where(slot == which, total_stat, 0.0), per_group)
        square = group_sum(jnp.where(slot == chunks + which, total_stat, 0.0), per_group)
        mean = total / members
        means.append(mean)
        invs.append(lax.rsqrt(square / members - mean * mean + EPSILON))
        at = pl.ds(pl.multiple_of(my_cols + k * LANES, LANES), LANES)
        gains.append(gain_ref[:, at])
        biases.append(bias_ref[:, at])

    def forward(rows, k):
        cols = slice(k * LANES, (k + 1) * LANES)
        normalized = (featc[rows, cols].astype(F32) - means[k]) * invs[k]
        normed = normalized * gains[k] + biases[k]
        return normalized, normed, 1.0 / (1.0 + jnp.exp(-normed))

    def activate(h, carry):
        rows = rows_of(h)
        for k in range(mine):
            _, normed, sig = forward(rows, k)
            act[1, rows, k * LANES:(k + 1) * LANES] = (normed * sig).astype(BF16)
        return carry

    lax.fori_loop(0, tall, activate, 0)

    tops_wait()
    gmax = jnp.max(tops[...].max(0), axis=1, keepdims=True)
    bound = GAIN_MAX * math.sqrt(float(pixels) * float(members)) + BIAS_MAX * pixels
    reach = bound * jnp.maximum(gmax, 1e-30) * (2.0 ** -13.9)
    scale = 1.0 / reach

    def shift(h, carry):
        rows = rows_of(h)
        for k in range(mine):
            cols = slice(k * LANES, (k + 1) * LANES)
            a = act[1, rows, cols].astype(F32)
            act[0, rows, cols] = from_left(a).astype(BF16)
            act[2, rows, cols] = from_right(a).astype(BF16)
        return carry

    def multiply(t):
        s = lax.rem(1 + 2 * lax.rem(t, 3), 3)
        r = lax.rem(1 + 2 * lax.div(t, 3), 3)
        start = pl.multiple_of((2 - r) * width, LANES)
        for m in range(2):
            result = jnp.dot(
                gt[m * half:(m + 1) * half, pl.ds(start, area)], act[s],
                preferred_element_type=F32,
            )
            part[t, m * (chips // 2):(m + 1) * (chips // 2)] = result.reshape(
                chips // 2, 2 * block, half
            )

    def reached(t, least):
        return lax.div(t + TAPS - least, TAPS)

    def swapped(t, k):
        return k * (1 - reached(t, SWAPPED))

    def order_of(t, k):
        if k == 0 or t >= SWAPPED:
            return list(range(bits))
        return [1, 2, 0] + list(range(3, bits)) if t < TURNED else [1, 0] + list(range(2, bits))

    def copy_a(t, k):
        kind = swapped(t, k)
        target = me + kind * across[1] + (1 - kind) * across[0]
        return remote(sa.at[t, k], ra.at[t, k], out_send.at[0], a_recv.at[t, k], target)

    def copy_b(t, k):
        target = me + across[order_of(t, k)[1]]
        return remote(sb.at[t, k], rb.at[t, k], out_send.at[1], b_recv.at[t, k], target)

    def copy_m(t, k, j):
        at = pl.ds(chips // 4 - (chips >> j), chips >> (j + 1))
        return remote(
            sm.at[t, k, at], rm.at[t, k, at],
            out_send.at[2], m_recv.at[t, k, j - 2], me + across[order_of(t, k)[j]],
        )

    def copy_c(t, k, way, source):
        target = lax.div(me + across[order_of(t, k)[-1]], 2) * 2 + way
        return remote(
            sc.at[t, k, way], rc.at[t, k, source],
            out_send.at[3], c_recv.at[t, k], target,
        )

    def copy_h(t, k):
        return remote(hs.at[t, k], hr.at[t, k], out_send.at[4], c_recv.at[t, k], mate)

    def lanes_of(k):
        return slice(k * LANES, (k + 1) * LANES)

    def stage_a(t, k):
        kind = swapped(t, k)
        for w in range(chips // 2):
            u, v = w >> 1, w & 1
            dest = u * 4 + kind * (2 * (1 - bit[1]) + v) + (1 - kind) * (2 * v + 1 - bit[0])
            sa[t, k, w] = encode(part[t, dest, :, lanes_of(k)] * scale)
        copy_a(t, k).start()

    def hop(t, k, i):
        order = order_of(t, k)
        before = sorted(set(range(bits)) - set(order[:i]))
        rest = [b for b in before if b != order[i]]
        here = bit[order[i]]
        if i == 1:
            copy_a(t, k).wait_recv()
            buffer, base = ra, 0
        elif i == 2:
            copy_b(t, k).wait_recv()
            buffer, base = rb, 0
        else:
            copy_m(t, k, i - 1).wait_recv()
            buffer, base = rm, chips // 4 - (chips >> (i - 1))

        def place(w, side):
            spot = side * (1 << order[i])
            for b in order[:i]:
                spot = spot + bit[b] * (1 << b)
            return spot + sum(((w >> j) & 1) << b for j, b in enumerate(rest))

        def value(w, side, rows):
            index = base + side * (1 << before.index(order[i]))
            index = index + sum(((w >> j) & 1) << before.index(b) for j, b in enumerate(rest))
            kept = part[t, place(w, side), rows, lanes_of(k)]
            kept = kept * scale if i == 1 else kept
            return kept + decode(buffer[t, k, index, rows])

        if i < bits - 1:
            out = sb if i == 1 else sm
            first_slot = 0 if i == 1 else chips // 4 - (chips >> i)
            for w in range(chips >> (i + 1)):
                out[t, k, first_slot + w] = encode(value(w, 1 - here, slice(None)))
            (copy_b(t, k) if i == 1 else copy_m(t, k, i)).start()
            for w in range(chips >> (i + 1)):
                part[t, place(w, here), :, lanes_of(k)] = value(w, here, slice(None))
            return
        for way in range(2):
            rows = slice(way * block, (way + 1) * block)
            sc[t, k, way] = encode(value(0, 1 - here, rows))
            copy_c(t, k, way, core).start()
        hs[t, k] = value(0, here, pl.ds(pl.multiple_of((1 - core) * block, block), block))
        copy_h(t, k).start()
        rows = pl.ds(pl.multiple_of(core * block, block), block)
        part[t, chip, rows, lanes_of(k)] = value(0, here, rows)

    def stage_d(t, k):
        tap = 3 * lax.rem(1 + 2 * lax.div(t, 3), 3) + lax.rem(1 + 2 * lax.rem(t, 3), 3)
        rows = pl.ds(pl.multiple_of(core * block, block), block)
        remote(both, both, out_send.at[3], c_recv.at[t, k], mate).wait_recv()
        total = part[t, chip, rows, lanes_of(k)]
        total = total + decode(rc[t, k, core])
        at = pl.ds(pl.multiple_of(my_cols + k * LANES, LANES), LANES)
        fg_ref[tap, :, at] = total * (reach / pixels)
        total = hr[t, k] + decode(rc[t, k, 1 - core])
        at = pl.ds(pl.multiple_of(mate_cols + k * LANES, LANES), LANES)
        fg_ref[tap, :, at] = total * (reach / pixels)

    def gradients():
        for k in range(mine):
            cols = lanes_of(k)

            def grad_step(h, carry):
                bias_sum, gain_sum = carry
                rows = rows_of(h)
                normalized, normed, sig = forward(rows, k)
                pre = gact[rows, cols] * (sig * (1.0 + normed * (1.0 - sig)))
                gact[rows, cols] = pre
                return (
                    bias_sum + pre.reshape(width // 8, 8, LANES).sum(0),
                    gain_sum + (pre * normalized).reshape(width // 8, 8, LANES).sum(0),
                )

            zero = jnp.zeros((8, LANES), F32)
            bias_sum, gain_sum = lax.fori_loop(0, tall, grad_step, (zero, zero))
            sums[me, k:k + 1, :] = bias_sum.sum(0, keepdims=True)
            sums[me, mine + k:mine + k + 1, :] = gain_sum.sum(0, keepdims=True)
        sums_start()

    push_gin = remote(gin_s, gin_r, push_send.at[2], push_recv.at[2], mate)

    def finish():
        sums_wait()
        everyone = sums[...].reshape(chips, 2, 2 * mine, LANES).sum(0)
        for c in range(2):
            for k in range(mine):
                sums_ref[c * mine + k:c * mine + k + 1, :] = everyone[c, k:k + 1]
                sums_ref[chunks + c * mine + k:chunks + c * mine + k + 1, :] = (
                    everyone[c, mine + k:mine + k + 1]
                )
                cols = lanes_of(c * mine + k)
                bias_row[:, cols] = everyone[c, k:k + 1]
                gain_row[:, cols] = everyone[c, mine + k:mine + k + 1]
        half_finish(1)
        push_gin.start()

    def half_finish(side):
        base = (1 - core if side else core) * height
        for k in range(mine):
            mean_grad = group_sum(
                gains[k] * sums_ref[pl.ds(core * mine + k, 1), :], per_group
            ) / members
            mean_cross = group_sum(
                gains[k] * sums_ref[pl.ds(chunks + core * mine + k, 1), :], per_group
            ) / members
            at = pl.ds(pl.multiple_of(my_cols + k * LANES, LANES), LANES)

            def final_step(h, carry):
                rows = rows_of(base + h)
                cols = lanes_of(k)
                normalized = (featc[rows, cols].astype(F32) - means[k]) * invs[k]
                result = invs[k] * (gact[rows, cols] * gains[k] - mean_grad - normalized * mean_cross)
                if side:
                    gin_s[rows_of(h), cols] = result.astype(BF16)
                else:
                    gin_ref[rows_of(h), at] = result.astype(BF16)
                return carry

            lax.fori_loop(0, height, final_step, 0)

    def relay_below():
        @pl.when((core == 1) & has_below)
        def _():
            to_above.wait_recv()
            pass_below.start()

    def relay_above():
        @pl.when((core == 0) & has_above)
        def _():
            to_below.wait_recv()
            pass_above.start()

    def edge_below():
        @pl.when((core == 0) & has_below)
        def _():
            pass_below.wait_recv()

        transpose(tall + 1)

    def edge_above():
        @pl.when((core == 1) & has_above)
        def _():
            pass_above.wait_recv()

        transpose(0)

    def shifts():
        lax.fori_loop(0, tall, shift, 0)

    named = {"shift": shifts, "relay_b": relay_below, "relay_a": relay_above,
        "edge_b": edge_below, "edge_a": edge_above, "grad": gradients, "fin1": finish,
        "fin0": functools.partial(half_finish, 0),
    }

    def perform(name):
        if name in named:
            return named[name]()
        if name.startswith("conv"):
            j = int(name[4:])
            return conv(j) if j < height else None
        t, k = int(name[1]), int(name[2])
        if name[0] == "b":
            hop(t, k, 1)
        elif name[0] == "c":
            for i in range(2, bits):
                hop(t, k, i)
        else:
            stage_d(t, k)

    def run(t, carry):
        multiply(t)
        for k in range(mine):
            stage_a(t, k)
        for step, names in enumerate(PLAN):
            if names:
                @pl.when(t == step)
                def _():
                    for name in names:
                        perform(name)
        return carry

    lax.fori_loop(0, TAPS, run, 0)
    for name in REST:
        perform(name)

    push_gin.wait_recv()

    def collect(h, carry):
        gin_ref[rows_of(h), pl.ds(mate_cols, half)] = gin_r[rows_of(h), :]
        return carry

    lax.fori_loop(0, height, collect, 0)

    for j, (source, target) in enumerate(((sa, ra), (sb, rb), (sm, rm), (sc, rc), (hs, hr))):
        if j != 2 or bits > 3:
            remote(source, target, out_send.at[j], out_send.at[j], mate).wait_send()
    push_feat.wait_send()
    push_gout.wait_send()
    push_gin.wait_send()
    stat_drain()
    tops_drain()
    sums_drain()

    @pl.when((core == 0) & has_above)
    def _():
        to_above.wait_send()
        pass_above.wait_send()

    @pl.when((core == 1) & has_below)
    def _():
        to_below.wait_send()
        pass_below.wait_send()


def hand_over(gin, fg, gain, bias, gin_out, fg_out, gain_out, bias_out, sem):
    copies = [
        pltpu.make_async_copy(source, target, sem.at[j])
        for j, (source, target) in enumerate(
            ((gin, gin_out), (fg, fg_out), (gain, gain_out), (bias, bias_out))
        )
    ]
    for copy in copies:
        copy.start()
    for copy in copies:
        copy.wait()


def local(n, features, grad_out, filters, norm_gain, norm_bias):
    height, width, channels = features.shape
    slab = height * width
    area, half = 2 * slab, channels // 2
    block, chips, chunks = channels // n, n // 2, channels // LANES
    mine = chunks // 2
    by_tap = filters.transpose(1, 2, 0, 3).reshape(TAPS, channels, channels)
    dma = pltpu.SemaphoreType.DMA
    hbm, vmem = pl.BlockSpec(memory_space=pltpu.HBM), pl.BlockSpec(memory_space=pltpu.VMEM)
    lots = dma((TAPS, mine))
    bits, middle = chips.bit_length() - 1, max(1, chips // 4 - 2)
    results = pl.pallas_call(
        functools.partial(kernel, n, height, width, channels),
        out_shape=(
            jax.ShapeDtypeStruct((slab, channels), BF16),
            jax.ShapeDtypeStruct((TAPS, block, channels), F32),
            jax.ShapeDtypeStruct((1, channels), F32),
            jax.ShapeDtypeStruct((1, channels), F32),
        ),
        in_specs=[hbm] * 5,
        out_specs=(vmem,) * 4,
        scratch_shapes=[
            pltpu.VMEM((slab, channels), BF16),
            pltpu.VMEM((area, half), BF16),
            pltpu.VMEM((area + 2 * width, channels), BF16),
            pltpu.VMEM((TAPS, channels, half), BF16),
            pltpu.VMEM((channels, area + 2 * width), BF16),
            pltpu.VMEM((3, area, half), BF16),
            pltpu.VMEM((area, half), F32),
            pltpu.VMEM((TAPS, chips, 2 * block, half), F32),
            pltpu.VMEM((TAPS, mine, chips // 2, 2 * block, LANES), BF16),
            pltpu.VMEM((TAPS, mine, chips // 2, 2 * block, LANES), BF16),
            pltpu.VMEM((TAPS, mine, chips // 4, 2 * block, LANES), BF16),
            pltpu.VMEM((TAPS, mine, chips // 4, 2 * block, LANES), BF16),
            pltpu.VMEM((TAPS, mine, middle, 2 * block, LANES), BF16),
            pltpu.VMEM((TAPS, mine, middle, 2 * block, LANES), BF16),
            pltpu.VMEM((TAPS, mine, 2, block, LANES), BF16),
            pltpu.VMEM((TAPS, mine, 2, block, LANES), BF16),
            pltpu.VMEM((TAPS, mine, block, LANES), F32),
            pltpu.VMEM((TAPS, mine, block, LANES), F32),
            pltpu.VMEM((2, block, LANES), F32),
            pltpu.VMEM((slab, half), BF16),
            pltpu.VMEM((slab, half), BF16),
            pltpu.VMEM((n, 1, LANES), F32),
            pltpu.VMEM((n, 1, LANES), F32),
            pltpu.VMEM((n, 2 * mine, LANES), F32),
            pltpu.VMEM((2 * chunks, LANES), F32),
            pltpu.VMEM((1, channels), F32),
            pltpu.VMEM((1, channels), F32),
            dma((height,)), dma((5,)), dma((3,)), dma((3,)), dma((2,)), dma((2,)),
            dma((3,)), dma((3,)),
            dma((5,)), lots, lots, dma((TAPS, mine, bits - 3) if bits > 3 else (1,)), lots,
        ],
        compiler_params=pltpu.CompilerParams(
            collective_id=0, has_side_effects=True, vmem_limit_bytes=MAIN * 1024 * 1024
        ),
        name="block_backward",
    )(
        *(
            pltpu.with_memory_space_constraint(x, pltpu.HBM)
            for x in (
                features.reshape(slab, channels), grad_out.reshape(slab, channels), by_tap,
                norm_gain.reshape(1, channels), norm_bias.reshape(1, channels),
            )
        ),
    )
    grad_in, filter_grad, gain_grad, bias_grad = pl.pallas_call(
        hand_over,
        out_shape=(
            jax.ShapeDtypeStruct((slab, channels), BF16),
            jax.ShapeDtypeStruct((TAPS, block, channels), F32),
            jax.ShapeDtypeStruct((1, channels), F32),
            jax.ShapeDtypeStruct((1, channels), F32),
        ),
        in_specs=[vmem] * 4,
        out_specs=(hbm,) * 4,
        scratch_shapes=[dma((4,))],
        compiler_params=pltpu.CompilerParams(vmem_limit_bytes=8 * 1024 * 1024),
        name="hand_over",
    )(*results)
    return (
        grad_in.reshape(height, width, channels),
        filter_grad.transpose(1, 0, 2).reshape(block, 3, 3, channels),
        gain_grad.reshape(channels),
        bias_grad.reshape(channels),
    )


def solution(mesh):
    slabs = P(("parts", "rows"), None, None)
    return jax.shard_map(
        functools.partial(local, mesh.shape["rows"]),
        mesh=mesh,
        in_specs=(slabs, slabs, P(), P(), P()),
        out_specs=(slabs, P(("parts", "rows"), None, None, None), P("parts"), P("parts")),
        check_vma=False,
    )
```

```python
import functools
import math

import jax
import jax.numpy as jnp
from jax import lax
from jax.experimental import pallas as pl
from jax.experimental.pallas import tpu as pltpu
from jax.sharding import PartitionSpec as P

GROUPS = 32
LANES = 128
POWER = 9
TAPS = 9
SWAPPED = 5
TURNED = 2
PLAN = (("shift", ), (), ("relay_b", "conv1", "edge_b", ), ("b00", "b01", ), ("b10", "b11", "relay_a", ), ("conv2", "b20", "edge_a", ), ("b30", "conv3", "b40", "c00", ), ("grad", "b50", "c10", "b51", ), ("b21", "b31", "b41", "c01", "c11", "b60", "c20", "c30", ))
REST = ("b61", "c40", "b70", "c50", "b71", "c51", "c60", "b80", "c61", "d00", "d10", "b81", "c70", "d20", "d30", "c21", "fin1", "c71", "c31", "c41", "fin0", "c80", "d40", "d50", "d51", "c81", "d60", "d61", "d01", "d11", "d70", "d21", "d71", "d31", "d41", "d80", "d81", )
MAIN = 40
EPSILON = 1e-06
GAIN_MAX = 1.75
BIAS_MAX = 1.0
MESH = pl.DeviceIdType.MESH
F32 = jnp.float32
BF16 = jnp.bfloat16


def encode(value):
    square = value * value
    fourth = square * square
    return (fourth * fourth * value).astype(BF16)


def decode(coded):
    wide = coded.astype(F32)
    root = jnp.exp2(jnp.log2(jnp.maximum(jnp.abs(wide), 1e-38)) * (1.0 / POWER))
    root = jnp.where(jnp.abs(wide) < 1e-37, 0.0, root)
    return jnp.where(wide < 0.0, -root, root)


def group_sum(row, per_group):
    value = jnp.broadcast_to(row, (8, LANES))
    lane = lax.broadcasted_iota(jnp.int32, (8, LANES), 1)
    step = 1
    while step < per_group:
        low = pltpu.roll(value, step, 1)
        high = pltpu.roll(value, LANES - step, 1)
        value = value + jnp.where((lane & step) != 0, low, high)
        step *= 2
    return value[0:1]


def kernel(
    n, height, width, channels,
    feat_hbm, gout_hbm, filt_hbm, gain_hbm, bias_hbm,
    gin_ref, fg_ref, gain_row, bias_row,
    feat, featc, gext, filt, gt, act, gact, part, sa, ra, sb, rb, sm, rm, sc, rc, hs, hr, both,
    gin_s, gin_r, stat, tops, sums, sums_ref, gain_ref, bias_ref,
    feat_sem, local_sem, push_send, push_recv, halo_send, halo_recv,
    share_send, share_recv,
    out_send, a_recv, b_recv, m_recv, c_recv,
):
    me = lax.axis_index("rows")
    core, chip = lax.rem(me, 2), lax.div(me, 2)
    mate = me + 1 - 2 * core
    chips = n // 2
    bits = chips.bit_length() - 1
    bit = [lax.rem(lax.div(chip, 1 << j), 2) for j in range(bits)]
    across = [(2 << j) * (1 - 2 * bit[j]) for j in range(bits)]
    block = channels // n
    half = channels // 2
    chunks = channels // LANES
    mine = half // LANES
    per_group = channels // GROUPS
    slab = height * width
    tall = 2 * height
    area = 2 * slab
    pixels = slab * n
    members = pixels * per_group
    own = pl.multiple_of(core * slab, slab)
    other = pl.multiple_of((1 - core) * slab, slab)
    my_cols = pl.multiple_of(core * half, LANES)
    mate_cols = pl.multiple_of((1 - core) * half, LANES)

    def remote(src, dst, send, recv, target):
        return pltpu.make_async_remote_copy(
            src_ref=src, dst_ref=dst, send_sem=send, recv_sem=recv,
            device_id={"rows": target}, device_id_type=MESH,
        )

    def peer(k):
        return lax.rem(me + k, n)

    def rows_of(h):
        return pl.ds(pl.multiple_of(h * width, width), width)

    in_feat = [
        pltpu.make_async_copy(
            feat_hbm.at[pl.ds(h * width, width)], feat.at[pl.ds(h * width, width)], feat_sem.at[h]
        )
        for h in range(height)
    ]
    in_gout = pltpu.make_async_copy(
        gout_hbm, gext.at[pl.ds(width + own, slab)], local_sem.at[0]
    )
    in_half = pltpu.make_async_copy(
        feat_hbm.at[:, pl.ds(my_cols, half)], featc.at[pl.ds(own, slab)], local_sem.at[1]
    )
    in_filt = pltpu.make_async_copy(
        filt_hbm.at[:, :, pl.ds(my_cols, half)], filt, local_sem.at[2]
    )
    in_gain = pltpu.make_async_copy(gain_hbm, gain_ref, local_sem.at[3])
    in_bias = pltpu.make_async_copy(bias_hbm, bias_ref, local_sem.at[4])
    for copy in in_feat:
        copy.start()

    barrier = pltpu.get_barrier_semaphore()

    def greet(k, carry):
        pl.semaphore_signal(barrier, inc=1, device_id={"rows": peer(k)}, device_id_type=MESH)
        return carry

    lax.fori_loop(1, n, greet, 0)

    in_gout.start()

    def shared(buffer, j):
        def copy(k):
            return remote(
                buffer.at[me], buffer.at[me], share_send.at[j], share_recv.at[j], peer(k)
            )

        def start():
            def body(k, carry):
                copy(k).start()
                return carry
            lax.fori_loop(1, n, body, 0)

        others = buffer.at[pl.ds(0, n - 1)]
        every = remote(others, others, share_send.at[j], share_recv.at[j], mate)
        return start, every.wait_recv, every.wait_send

    stat_start, stat_wait, stat_drain = shared(stat, 0)
    tops_start, tops_wait, tops_drain = shared(tops, 1)
    sums_start, sums_wait, sums_drain = shared(sums, 2)

    lane = lax.broadcasted_iota(jnp.int32, (1, LANES), 1)
    slot = lane & (per_group - 1)
    totals = [jnp.zeros((8, LANES), F32) for _ in range(chunks)]
    squares = [jnp.zeros((8, LANES), F32) for _ in range(chunks)]
    for h in range(height):
        in_feat[h].wait()
        for c in range(chunks):
            x = feat[h * width:(h + 1) * width, c * LANES:(c + 1) * LANES].astype(F32)
            x = x.reshape(width // 8, 8, LANES)
            totals[c] = totals[c] + x.sum(0)
            squares[c] = squares[c] + (x * x).sum(0)
    in_half.start()
    in_filt.start()
    in_gain.start()
    in_bias.start()
    packed = jnp.zeros((1, LANES), F32)
    for c in range(chunks):
        total = group_sum(totals[c].sum(0, keepdims=True), per_group)
        square = group_sum(squares[c].sum(0, keepdims=True), per_group)
        packed = packed + jnp.where(slot == c, total, 0.0)
        packed = packed + jnp.where(slot == chunks + c, square, 0.0)
    stat[me] = packed

    in_gout.wait()

    def top_step(h, carry):
        g = jnp.abs(gext[rows_of(1 + core * height + h), :])
        return jnp.maximum(carry, g.reshape(width // 16, 16, channels).max(0))

    largest = lax.fori_loop(0, height, top_step, jnp.zeros((16, channels), BF16))
    largest = largest.astype(F32).max(0, keepdims=True)
    top = jnp.zeros((1, LANES), F32)
    for c in range(chunks):
        top = jnp.maximum(top, largest[:, c * LANES:(c + 1) * LANES])
    tops[me] = top
    push_feat = remote(
        feat.at[:, pl.ds(mate_cols, half)], featc.at[pl.ds(own, slab)],
        push_send.at[0], push_recv.at[0], mate,
    )
    push_gout = remote(
        gext.at[pl.ds(width + own, slab)], gext.at[pl.ds(width + own, slab)],
        push_send.at[1], push_recv.at[1], mate,
    )
    pl.semaphore_wait(barrier, n - 1)
    stat_start()
    tops_start()
    push_gout.start()
    push_feat.start()

    above, below = pl.ds(0, width), pl.ds((tall + 1) * width, width)
    first, last = pl.ds(width, width), pl.ds(tall * width, width)

    to_above = remote(gext.at[first], gext.at[below], halo_send.at[0], halo_recv.at[0], me - 1)
    to_below = remote(gext.at[last], gext.at[above], halo_send.at[0], halo_recv.at[0], me + 1)
    pass_above = remote(gext.at[above], gext.at[above], halo_send.at[1], halo_recv.at[1], mate)
    pass_below = remote(gext.at[below], gext.at[below], halo_send.at[1], halo_recv.at[1], mate)
    has_above, has_below = chip > 0, chip < chips - 1

    @pl.when(chip == 0)
    def _():
        gext[above, :] = jnp.zeros((width, channels), BF16)

    @pl.when(chip == chips - 1)
    def _():
        gext[below, :] = jnp.zeros((width, channels), BF16)


    @pl.when((core == 0) & has_above)
    def _():
        to_above.start()

    @pl.when((core == 1) & has_below)
    def _():
        to_below.start()


    column = lax.broadcasted_iota(jnp.int32, (width, LANES), 0)

    def from_left(x):
        return jnp.where(column > 0, pltpu.roll(x, 1, 0), 0.0)

    def from_right(x):
        return jnp.where(column < width - 1, pltpu.roll(x, width - 1, 0), 0.0)

    def conv(j):
        turned = core * (height - 2 - 2 * j) + j
        inner = lax.div(height - 1 - j + tall - 3, tall - 2)
        first_row = 1 + 2 * (inner * turned + (1 - inner) * j)
        where = [first_row, lax.rem(first_row + 1, tall)]
        ys = [[], []]
        for s in range(3):
            for m in range(2):
                y = None
                for r in range(3):
                    d = jnp.dot(
                        gext[rows_of(where[m] - r + 2), :], filt[3 * r + s],
                        preferred_element_type=F32,
                    )
                    y = d if y is None else y + d
                ys[m].append(y)
        for m in range(2):
            for k in range(mine):
                sub = slice(k * LANES, (k + 1) * LANES)
                y = ys[m]
                gact[rows_of(where[m]), sub] = (
                    y[1][:, sub] + from_right(y[0][:, sub]) + from_left(y[2][:, sub])
                )

    def transpose(e):
        start = pl.multiple_of(e * width, width)
        gt[:, pl.ds(start, width)] = gext[pl.ds(start, width), :].T

    def transposes(base, count):
        def body(e, carry):
            transpose(base + e)
            return carry
        lax.fori_loop(0, count, body, 0)

    transposes(1 + core * height, height)
    in_filt.wait()
    conv(0)

    push_gout_in = remote(
        gext.at[pl.ds(width + other, slab)], gext.at[pl.ds(width + other, slab)],
        push_send.at[1], push_recv.at[1], mate,
    )
    push_feat_in = remote(
        feat.at[:, pl.ds(mate_cols, half)], featc.at[pl.ds(other, slab)],
        push_send.at[0], push_recv.at[0], mate,
    )
    push_gout_in.wait_recv()
    transposes(1 + (1 - core) * height, height)

    in_half.wait()
    in_gain.wait()
    in_bias.wait()
    push_feat_in.wait_recv()

    stat_wait()
    total_stat = stat[...].sum(0)
    means, invs, gains, biases = [], [], [], []
    for k in range(mine):
        which = core * mine + k
        total = group_sum(jnp.where(slot == which, total_stat, 0.0), per_group)
        square = group_sum(jnp.where(slot == chunks + which, total_stat, 0.0), per_group)
        mean = total / members
        means.append(mean)
        invs.append(lax.rsqrt(square / members - mean * mean + EPSILON))
        at = pl.ds(pl.multiple_of(my_cols + k * LANES, LANES), LANES)
        gains.append(gain_ref[:, at])
        biases.append(bias_ref[:, at])

    def forward(rows, k):
        cols = slice(k * LANES, (k + 1) * LANES)
        normalized = (featc[rows, cols].astype(F32) - means[k]) * invs[k]
        normed = normalized * gains[k] + biases[k]
        return normalized, normed, 1.0 / (1.0 + jnp.exp(-normed))

    def activate(h, carry):
        rows = rows_of(h)
        for k in range(mine):
            _, normed, sig = forward(rows, k)
            act[1, rows, k * LANES:(k + 1) * LANES] = (normed * sig).astype(BF16)
        return carry

    lax.fori_loop(0, tall, activate, 0)

    tops_wait()
    gmax = jnp.max(tops[...].max(0), axis=1, keepdims=True)
    bound = GAIN_MAX * math.sqrt(float(pixels) * float(members)) + BIAS_MAX * pixels
    reach = bound * jnp.maximum(gmax, 1e-30) * (2.0 ** -13.9)
    scale = 1.0 / reach

    def shift(h, carry):
        rows = rows_of(h)
        for k in range(mine):
            cols = slice(k * LANES, (k + 1) * LANES)
            a = act[1, rows, cols].astype(F32)
            act[0, rows, cols] = from_left(a).astype(BF16)
            act[2, rows, cols] = from_right(a).astype(BF16)
        return carry

    def multiply(t):
        s = lax.rem(1 + 2 * lax.rem(t, 3), 3)
        r = lax.rem(1 + 2 * lax.div(t, 3), 3)
        start = pl.multiple_of((2 - r) * width, LANES)
        for m in range(2):
            result = jnp.dot(
                gt[m * half:(m + 1) * half, pl.ds(start, area)], act[s],
                preferred_element_type=F32,
            )
            part[t, m * (chips // 2):(m + 1) * (chips // 2)] = result.reshape(
                chips // 2, 2 * block, half
            )

    def reached(t, least):
        return lax.div(t + TAPS - least, TAPS)

    def swapped(t, k):
        return k * (1 - reached(t, SWAPPED))

    def order_of(t, k):
        if k == 0 or t >= SWAPPED:
            return list(range(bits))
        return [1, 2, 0] + list(range(3, bits)) if t < TURNED else [1, 0] + list(range(2, bits))

    def copy_a(t, k):
        kind = swapped(t, k)
        target = me + kind * across[1] + (1 - kind) * across[0]
        return remote(sa.at[t, k], ra.at[t, k], out_send.at[0], a_recv.at[t, k], target)

    def copy_b(t, k):
        target = me + across[order_of(t, k)[1]]
        return remote(sb.at[t, k], rb.at[t, k], out_send.at[1], b_recv.at[t, k], target)

    def copy_m(t, k, j):
        at = pl.ds(chips // 4 - (chips >> j), chips >> (j + 1))
        return remote(
            sm.at[t, k, at], rm.at[t, k, at],
            out_send.at[2], m_recv.at[t, k, j - 2], me + across[order_of(t, k)[j]],
        )

    def copy_c(t, k, way, source):
        target = lax.div(me + across[order_of(t, k)[-1]], 2) * 2 + way
        return remote(
            sc.at[t, k, way], rc.at[t, k, source],
            out_send.at[3], c_recv.at[t, k], target,
        )

    def copy_h(t, k):
        return remote(hs.at[t, k], hr.at[t, k], out_send.at[4], c_recv.at[t, k], mate)

    def lanes_of(k):
        return slice(k * LANES, (k + 1) * LANES)

    def stage_a(t, k):
        kind = swapped(t, k)
        for w in range(chips // 2):
            u, v = w >> 1, w & 1
            dest = u * 4 + kind * (2 * (1 - bit[1]) + v) + (1 - kind) * (2 * v + 1 - bit[0])
            sa[t, k, w] = encode(part[t, dest, :, lanes_of(k)] * scale)
        copy_a(t, k).start()

    def hop(t, k, i):
        order = order_of(t, k)
        before = sorted(set(range(bits)) - set(order[:i]))
        rest = [b for b in before if b != order[i]]
        here = bit[order[i]]
        if i == 1:
            copy_a(t, k).wait_recv()
            buffer, base = ra, 0
        elif i == 2:
            copy_b(t, k).wait_recv()
            buffer, base = rb, 0
        else:
            copy_m(t, k, i - 1).wait_recv()
            buffer, base = rm, chips // 4 - (chips >> (i - 1))

        def place(w, side):
            spot = side * (1 << order[i])
            for b in order[:i]:
                spot = spot + bit[b] * (1 << b)
            return spot + sum(((w >> j) & 1) << b for j, b in enumerate(rest))

        def value(w, side, rows):
            index = base + side * (1 << before.index(order[i]))
            index = index + sum(((w >> j) & 1) << before.index(b) for j, b in enumerate(rest))
            kept = part[t, place(w, side), rows, lanes_of(k)]
            kept = kept * scale if i == 1 else kept
            return kept + decode(buffer[t, k, index, rows])

        if i < bits - 1:
            out = sb if i == 1 else sm
            first_slot = 0 if i == 1 else chips // 4 - (chips >> i)
            for w in range(chips >> (i + 1)):
                out[t, k, first_slot + w] = encode(value(w, 1 - here, slice(None)))
            (copy_b(t, k) if i == 1 else copy_m(t, k, i)).start()
            for w in range(chips >> (i + 1)):
                part[t, place(w, here), :, lanes_of(k)] = value(w, here, slice(None))
            return
        for way in range(2):
            rows = slice(way * block, (way + 1) * block)
            sc[t, k, way] = encode(value(0, 1 - here, rows))
            copy_c(t, k, way, core).start()
        hs[t, k] = value(0, here, pl.ds(pl.multiple_of((1 - core) * block, block), block))
        copy_h(t, k).start()
        rows = pl.ds(pl.multiple_of(core * block, block), block)
        part[t, chip, rows, lanes_of(k)] = value(0, here, rows)

    def stage_d(t, k):
        tap = 3 * lax.rem(1 + 2 * lax.div(t, 3), 3) + lax.rem(1 + 2 * lax.rem(t, 3), 3)
        rows = pl.ds(pl.multiple_of(core * block, block), block)
        remote(both, both, out_send.at[3], c_recv.at[t, k], mate).wait_recv()
        total = part[t, chip, rows, lanes_of(k)]
        total = total + decode(rc[t, k, core])
        at = pl.ds(pl.multiple_of(my_cols + k * LANES, LANES), LANES)
        fg_ref[tap, :, at] = total * (reach / pixels)
        total = hr[t, k] + decode(rc[t, k, 1 - core])
        at = pl.ds(pl.multiple_of(mate_cols + k * LANES, LANES), LANES)
        fg_ref[tap, :, at] = total * (reach / pixels)

    def gradients():
        for k in range(mine):
            cols = lanes_of(k)

            def grad_step(h, carry):
                bias_sum, gain_sum = carry
                rows = rows_of(h)
                normalized, normed, sig = forward(rows, k)
                pre = gact[rows, cols] * (sig * (1.0 + normed * (1.0 - sig)))
                gact[rows, cols] = pre
                return (
                    bias_sum + pre.reshape(width // 8, 8, LANES).sum(0),
                    gain_sum + (pre * normalized).reshape(width // 8, 8, LANES).sum(0),
                )

            zero = jnp.zeros((8, LANES), F32)
            bias_sum, gain_sum = lax.fori_loop(0, tall, grad_step, (zero, zero))
            sums[me, k:k + 1, :] = bias_sum.sum(0, keepdims=True)
            sums[me, mine + k:mine + k + 1, :] = gain_sum.sum(0, keepdims=True)
        sums_start()

    push_gin = remote(gin_s, gin_r, push_send.at[2], push_recv.at[2], mate)

    def finish():
        sums_wait()
        everyone = sums[...].reshape(chips, 2, 2 * mine, LANES).sum(0)
        for c in range(2):
            for k in range(mine):
                sums_ref[c * mine + k:c * mine + k + 1, :] = everyone[c, k:k + 1]
                sums_ref[chunks + c * mine + k:chunks + c * mine + k + 1, :] = (
                    everyone[c, mine + k:mine + k + 1]
                )
                cols = lanes_of(c * mine + k)
                bias_row[:, cols] = everyone[c, k:k + 1]
                gain_row[:, cols] = everyone[c, mine + k:mine + k + 1]
        half_finish(1)
        push_gin.start()

    def half_finish(side):
        base = (1 - core if side else core) * height
        for k in range(mine):
            mean_grad = group_sum(
                gains[k] * sums_ref[pl.ds(core * mine + k, 1), :], per_group
            ) / members
            mean_cross = group_sum(
                gains[k] * sums_ref[pl.ds(chunks + core * mine + k, 1), :], per_group
            ) / members
            at = pl.ds(pl.multiple_of(my_cols + k * LANES, LANES), LANES)

            def final_step(h, carry):
                rows = rows_of(base + h)
                cols = lanes_of(k)
                normalized = (featc[rows, cols].astype(F32) - means[k]) * invs[k]
                result = invs[k] * (gact[rows, cols] * gains[k] - mean_grad - normalized * mean_cross)
                if side:
                    gin_s[rows_of(h), cols] = result.astype(BF16)
                else:
                    gin_ref[rows_of(h), at] = result.astype(BF16)
                return carry

            lax.fori_loop(0, height, final_step, 0)

    def relay_below():
        @pl.when((core == 1) & has_below)
        def _():
            to_above.wait_recv()
            pass_below.start()

    def relay_above():
        @pl.when((core == 0) & has_above)
        def _():
            to_below.wait_recv()
            pass_above.start()

    def edge_below():
        @pl.when((core == 0) & has_below)
        def _():
            pass_below.wait_recv()

        transpose(tall + 1)

    def edge_above():
        @pl.when((core == 1) & has_above)
        def _():
            pass_above.wait_recv()

        transpose(0)

    def shifts():
        lax.fori_loop(0, tall, shift, 0)

    named = {"shift": shifts, "relay_b": relay_below, "relay_a": relay_above,
        "edge_b": edge_below, "edge_a": edge_above, "grad": gradients, "fin1": finish,
        "fin0": functools.partial(half_finish, 0),
    }

    def perform(name):
        if name in named:
            return named[name]()
        if name.startswith("conv"):
            j = int(name[4:])
            return conv(j) if j < height else None
        t, k = int(name[1]), int(name[2])
        if name[0] == "b":
            hop(t, k, 1)
        elif name[0] == "c":
            for i in range(2, bits):
                hop(t, k, i)
        else:
            stage_d(t, k)

    def run(t, carry):
        multiply(t)
        for k in range(mine):
            stage_a(t, k)
        for step, names in enumerate(PLAN):
            if names:
                @pl.when(t == step)
                def _():
                    for name in names:
                        perform(name)
        return carry

    lax.fori_loop(0, TAPS, run, 0)
    for name in REST:
        perform(name)

    push_gin.wait_recv()

    def collect(h, carry):
        gin_ref[rows_of(h), pl.ds(mate_cols, half)] = gin_r[rows_of(h), :]
        return carry

    lax.fori_loop(0, height, collect, 0)

    for j, (source, target) in enumerate(((sa, ra), (sb, rb), (sm, rm), (sc, rc), (hs, hr))):
        if j != 2 or bits > 3:
            remote(source, target, out_send.at[j], out_send.at[j], mate).wait_send()
    push_feat.wait_send()
    push_gout.wait_send()
    push_gin.wait_send()
    stat_drain()
    tops_drain()
    sums_drain()

    @pl.when((core == 0) & has_above)
    def _():
        to_above.wait_send()
        pass_above.wait_send()

    @pl.when((core == 1) & has_below)
    def _():
        to_below.wait_send()
        pass_below.wait_send()


def hand_over(gin, fg, gain, bias, gin_out, fg_out, gain_out, bias_out, sem):
    copies = [
        pltpu.make_async_copy(source, target, sem.at[j])
        for j, (source, target) in enumerate(
            ((gin, gin_out), (fg, fg_out), (gain, gain_out), (bias, bias_out))
        )
    ]
    for copy in copies:
        copy.start()
    for copy in copies:
        copy.wait()


def local(n, features, grad_out, filters, norm_gain, norm_bias):
    height, width, channels = features.shape
    slab = height * width
    area, half = 2 * slab, channels // 2
    block, chips, chunks = channels // n, n // 2, channels // LANES
    mine = chunks // 2
    by_tap = filters.transpose(1, 2, 0, 3).reshape(TAPS, channels, channels)
    dma = pltpu.SemaphoreType.DMA
    hbm, vmem = pl.BlockSpec(memory_space=pltpu.HBM), pl.BlockSpec(memory_space=pltpu.VMEM)
    lots = dma((TAPS, mine))
    bits, middle = chips.bit_length() - 1, max(1, chips // 4 - 2)
    results = pl.pallas_call(
        functools.partial(kernel, n, height, width, channels),
        out_shape=(
            jax.ShapeDtypeStruct((slab, channels), BF16),
            jax.ShapeDtypeStruct((TAPS, block, channels), F32),
            jax.ShapeDtypeStruct((1, channels), F32),
            jax.ShapeDtypeStruct((1, channels), F32),
        ),
        in_specs=[hbm] * 5,
        out_specs=(vmem,) * 4,
        scratch_shapes=[
            pltpu.VMEM((slab, channels), BF16),
            pltpu.VMEM((area, half), BF16),
            pltpu.VMEM((area + 2 * width, channels), BF16),
            pltpu.VMEM((TAPS, channels, half), BF16),
            pltpu.VMEM((channels, area + 2 * width), BF16),
            pltpu.VMEM((3, area, half), BF16),
            pltpu.VMEM((area, half), F32),
            pltpu.VMEM((TAPS, chips, 2 * block, half), F32),
            pltpu.VMEM((TAPS, mine, chips // 2, 2 * block, LANES), BF16),
            pltpu.VMEM((TAPS, mine, chips // 2, 2 * block, LANES), BF16),
            pltpu.VMEM((TAPS, mine, chips // 4, 2 * block, LANES), BF16),
            pltpu.VMEM((TAPS, mine, chips // 4, 2 * block, LANES), BF16),
            pltpu.VMEM((TAPS, mine, middle, 2 * block, LANES), BF16),
            pltpu.VMEM((TAPS, mine, middle, 2 * block, LANES), BF16),
            pltpu.VMEM((TAPS, mine, 2, block, LANES), BF16),
            pltpu.VMEM((TAPS, mine, 2, block, LANES), BF16),
            pltpu.VMEM((TAPS, mine, block, LANES), F32),
            pltpu.VMEM((TAPS, mine, block, LANES), F32),
            pltpu.VMEM((2, block, LANES), F32),
            pltpu.VMEM((slab, half), BF16),
            pltpu.VMEM((slab, half), BF16),
            pltpu.VMEM((n, 1, LANES), F32),
            pltpu.VMEM((n, 1, LANES), F32),
            pltpu.VMEM((n, 2 * mine, LANES), F32),
            pltpu.VMEM((2 * chunks, LANES), F32),
            pltpu.VMEM((1, channels), F32),
            pltpu.VMEM((1, channels), F32),
            dma((height,)), dma((5,)), dma((3,)), dma((3,)), dma((2,)), dma((2,)),
            dma((3,)), dma((3,)),
            dma((5,)), lots, lots, dma((TAPS, mine, bits - 3) if bits > 3 else (1,)), lots,
        ],
        compiler_params=pltpu.CompilerParams(
            collective_id=0, has_side_effects=True, vmem_limit_bytes=MAIN * 1024 * 1024
        ),
        name="block_backward",
    )(
        *(
            pltpu.with_memory_space_constraint(x, pltpu.HBM)
            for x in (
                features.reshape(slab, channels), grad_out.reshape(slab, channels), by_tap,
                norm_gain.reshape(1, channels), norm_bias.reshape(1, channels),
            )
        ),
    )
    grad_in, filter_grad, gain_grad, bias_grad = pl.pallas_call(
        hand_over,
        out_shape=(
            jax.ShapeDtypeStruct((slab, channels), BF16),
            jax.ShapeDtypeStruct((TAPS, block, channels), F32),
            jax.ShapeDtypeStruct((1, channels), F32),
            jax.ShapeDtypeStruct((1, channels), F32),
        ),
        in_specs=[vmem] * 4,
        out_specs=(hbm,) * 4,
        scratch_shapes=[dma((4,))],
        compiler_params=pltpu.CompilerParams(vmem_limit_bytes=8 * 1024 * 1024),
        name="hand_over",
    )(*results)
    return (
        grad_in.reshape(height, width, channels),
        filter_grad.transpose(1, 0, 2).reshape(block, 3, 3, channels),
        gain_grad.reshape(channels),
        bias_grad.reshape(channels),
    )


def solution(mesh):
    slabs = P(("parts", "rows"), None, None)
    return jax.shard_map(
        functools.partial(local, mesh.shape["rows"]),
        mesh=mesh,
        in_specs=(slabs, slabs, P(), P(), P()),
        out_specs=(slabs, P(("parts", "rows"), None, None, None), P("parts"), P("parts")),
        check_vma=False,
    )
```
